256 devices in a mesh: gx: 32 (over z, x_lo, core), gy: 8 (over x_hi, y).
Axes of the slice: x: 4 (x_hi: 2, x_lo: 2; x = x_hi * 2 + x_lo), y: 4, z: 8, core: 2. Of those that a mesh axis runs over, the one named last changes fastest.
Arguments:
- volt: float32 [256, 512, 2048], P('gx', 'gy'), may hold values from -6 to 6
- drive: float32 [256, 512, 2048], P('gx', 'gy'), may hold values from -6 to 6
- region: int32 [256, 512, 32], P('gx', 'gy'), may hold values from 0 to 7
- diode_mask: int32 [256, 512, 32], P('gx', 'gy'), may hold values 0 or 1
- sigma_table: float32 [8], replicated, may hold values from 0.3 to 3
- cap_table: float32 [8], replicated, may hold values from 0.1 to 1
Outputs:
- residual: float32 [256, 512, 2048], P('gx', 'gy')
- coef_norms: float32 [64], replicated
The draws below stay inside these ranges and needn't reach their ends.
All inputs are finite; a program needn't handle non-finite values. No bound on the sum of `diode_mask` on one device may be relied on, other than what follows from the above.
Results may differ from the reference program's by a relative error of at most 0.0003.
Values sent between devices are 32-bit elements; how exact they have to be, the bound alone decides.
No kernel may reach another device: no remote copies, remote signals or barrier semaphores. Data moves between devices by JAX's collectives and lax.ppermute only.
A program may use at most 192 MiB of HBM per device.

```python
import math
import jax
import jax.numpy as jnp
from jax import lax

NZ = 32
H = 32
KC = 64
S = 256
REGIONS = 8
NX = 256
NY = 512


def with_ends(values, key, least, high):
    extent = values.shape
    place = [jax.random.randint(jax.random.fold_in(key, axis), (), 0, extent[axis]) for axis in range(len(extent))]
    values = values.at[tuple(place)].set(least)
    longest = extent.index(max(extent))
    place[longest] = (place[longest] + 1) % extent[longest]
    return values.at[tuple(place)].set(high)


def shard_levels(rng, shape, shards, least, high):
    def one(dim, shards_of):
        draws = jax.random.uniform(jax.random.fold_in(jax.random.fold_in(rng, 6), dim), (shards_of,), jnp.float32, least / len(shards), high / len(shards))
        return jnp.repeat(jnp.exp(draws), shape[dim] // shards_of).reshape((-1,) + (1,) * (len(shape) - dim - 1))

    loudness = one(*shards[0])
    for cut in shards[1:]:
        loudness = loudness * one(*cut)
    return loudness


def noise(stream_key, shape, spread, bound, pieces=(), held_as=jnp.bfloat16):
    gain = shard_levels(stream_key, shape, pieces, -0.22, 0.18) if pieces else 1.0
    entries = jax.random.normal(stream_key, shape, jnp.float32) * spread * gain
    return jnp.minimum(jnp.maximum(entries, -bound), bound).astype(held_as)


def setup_inputs(seed: int = 0) -> dict:
    key_of = jax.random.split(jax.random.key(seed), 7)
    return {
        "volt": noise(key_of[0], (NX, NY, NZ * KC), 1.0, 6.0, ((0, 32), (1, 8)), jnp.float32),
        "drive": noise(key_of[1], (NX, NY, NZ * KC), 1.0, 6.0, ((0, 32), (1, 8)), jnp.float32),
        "region": with_ends(jax.random.randint(key_of[2], (NX, NY, NZ), 0, REGIONS), jax.random.fold_in(key_of[2], 1), 0, REGIONS - 1).astype(jnp.int32),
        "diode_mask": with_ends((jax.random.randint(key_of[3], (NX, NY, NZ), 0, 4) < 1).astype(jnp.int32), jax.random.fold_in(key_of[3], 1), 0, 1),
        "sigma_table": jnp.clip(jnp.exp(jax.random.uniform(key_of[4], (REGIONS,), jnp.float32, math.log(0.3), math.log(3.0))), 0.3, 3.0),
        "cap_table": jnp.clip(jnp.exp(jax.random.uniform(key_of[5], (REGIONS,), jnp.float32, math.log(0.1), math.log(1.0))), 0.1, 1.0),
    }


base_freq = 0.1
norm_eps = 1e-06

def cut_slab(array, first_idx, last_idx, along):
    return lax.slice_in_dim(array, first_idx, last_idx, axis=along)

def harmonic_mean(left, right):
    return 2.0 * left * right / (left + right)

def open_terms(volt_field, conduct, along):
    cell_count = volt_field.shape[along]
    widths = [(0, 0)] * volt_field.ndim
    widths[along] = (1, 1)
    padded_volt = jnp.pad(volt_field, widths)
    padded_cond = jnp.pad(conduct, widths)
    face_flux = harmonic_mean(cut_slab(padded_cond, 0, cell_count + 1, along), cut_slab(padded_cond, 1, cell_count + 2, along)) * (cut_slab(padded_volt, 1, cell_count + 2, along) - cut_slab(padded_volt, 0, cell_count + 1, along))
    return cut_slab(face_flux, 0, cell_count, along) - cut_slab(face_flux, 1, cell_count + 1, along)

def time_derivative(coefs):
    half_count = coefs.shape[-1] // 2
    orders = base_freq * jnp.arange(1, half_count + 1, dtype=jnp.float32)
    return jnp.concatenate([orders * coefs[..., half_count:], -orders * coefs[..., :half_count]], axis=-1)

def spectral_tables(harmonics, samples):
    orders = jnp.arange(1, harmonics + 1, dtype=jnp.float32)
    times = 2.0 * math.pi * jnp.arange(samples, dtype=jnp.float32) / samples
    angles = orders[:, None] * times[None, :]
    synthesis = jnp.concatenate([jnp.cos(angles), jnp.sin(angles)], axis=0)
    analysis = synthesis.T * (2.0 / samples)
    return (synthesis, analysis)

def nonlinear_row(volt_row, diode_row, synthesis, analysis):
    coef_count = volt_row.shape[-1]
    flat = volt_row.reshape(-1, coef_count)
    cell_count = flat.shape[0]
    samples = jnp.dot(flat, synthesis, precision=lax.Precision.HIGHEST, preferred_element_type=jnp.float32)
    current = jax.nn.softplus(2.0 * samples) * 0.5
    charge = jnp.tanh(samples) * 0.5
    projected = jnp.dot(jnp.concatenate([current, charge], axis=0), analysis, precision=lax.Precision.HIGHEST, preferred_element_type=jnp.float32)
    combined = projected[:cell_count] + time_derivative(projected[cell_count:])
    return combined.reshape(volt_row.shape) * diode_row[..., None]

def reference(volt, drive, region, diode_mask, sigma_table, cap_table):
    conduct = jnp.take(sigma_table, region)[..., None]
    capacity = jnp.take(cap_table, region)[..., None]
    volt_field = volt.reshape(NX, NY, NZ, KC)
    drive_field = drive.reshape(NX, NY, NZ, KC)
    diode_field = diode_mask.astype(jnp.float32)
    synthesis, analysis = spectral_tables(H, S)

    def picker(array, row_index):
        return lax.dynamic_index_in_dim(array, row_index, 0, keepdims=False)

    def one_row(row_index):
        prev_row = (row_index - 1 + NX) % NX
        next_row = (row_index + 1) % NX
        volt_here = picker(volt_field, row_index)
        cond_here = picker(conduct, row_index)
        volt_prev = picker(volt_field, prev_row)
        cond_prev = picker(conduct, prev_row)
        volt_next = picker(volt_field, next_row)
        cond_next = picker(conduct, next_row)
        below_flux = harmonic_mean(cond_prev, cond_here) * (volt_here - volt_prev)
        above_flux = harmonic_mean(cond_here, cond_next) * (volt_next - volt_here)
        row_terms = below_flux - above_flux
        col_terms = open_terms(volt_here, cond_here, 0)
        depth_terms = open_terms(volt_here, cond_here, 1)
        diode_part = nonlinear_row(volt_here, picker(diode_field, row_index), synthesis, analysis)
        residual = row_terms + col_terms + depth_terms + picker(capacity, row_index) * time_derivative(volt_here) + diode_part - picker(drive_field, row_index)
        return (residual, lax.optimization_barrier(jnp.sum(residual * residual, axis=(0, 1))))
    residual, row_squares = lax.map(one_row, jnp.arange(NX, dtype=jnp.int32))
    summed = lax.optimization_barrier(jnp.sum(row_squares, axis=0))
    norms_out = jnp.sqrt(summed / (NX * NY * NZ) + norm_eps)
    return (residual.reshape(NX, NY, NZ * KC), norms_out)
```

```python
import functools
import math

import jax
import jax.numpy as jnp
import numpy as np
from jax import lax
from jax.experimental import pallas as pl
from jax.experimental.pallas import tpu as pltpu
from jax.sharding import PartitionSpec as P

NZ = 32
H = 32
KC = 64
S = 256
REGIONS = 8
ROWS = 8
COLS = 64
PAIRS = NZ // 2
LANES = 128
GROUPS = ROWS * COLS // LANES
CELLS = ROWS * COLS

base_freq = 0.1
norm_eps = 1e-06

GX = 0
GYP = GX + GROUPS + 1
GYM = GYP + GROUPS
GYH = GYM + GROUPS
GZP = GYH + GROUPS
GZM = GZP + GROUPS
CAP = GZM + GROUPS
DIO = CAP + GROUPS
GSUM = DIO + GROUPS
FIELDS = GSUM + GROUPS


def halves(table):
    high = table.astype(jnp.bfloat16)
    low = (table - high.astype(np.float64)).astype(jnp.bfloat16)
    return high, low


def constant_tables():
    orders = np.arange(1, H + 1, dtype=np.float64)
    angles = orders[:, None] * (2.0 * math.pi * np.arange(S) / S)[None, :]
    cosines, sines = np.cos(angles), np.sin(angles)
    synthesis = np.concatenate([cosines, sines], axis=0)
    high, low = halves(synthesis.T)
    forward = np.concatenate([high, low, high, low], axis=1)
    scaled = base_freq * orders[:, None]
    from_even = synthesis / S
    from_odd = np.concatenate([scaled * sines, -scaled * cosines], axis=0) / S
    even_high, even_low = halves(from_even)
    odd_high, odd_low = halves(from_odd)
    backward = np.concatenate(
        [
            np.concatenate([even_high, even_high, odd_high, odd_high], axis=1),
            np.concatenate([even_low, even_low, odd_low, odd_low], axis=1),
        ],
        axis=0,
    )
    rates = np.concatenate([scaled, -scaled], axis=0).astype(np.float32)
    spread = np.zeros((16, CELLS), np.float32)
    for row in range(ROWS):
        group, half = row % GROUPS, row // GROUPS
        spread[row, group * LANES + half * COLS] = 1.0
        spread[ROWS + row, group * LANES + half * COLS + COLS - 1] = 1.0
    return forward, backward, rates, spread


def split(values):
    high = values.astype(jnp.bfloat16)
    low = (values - high.astype(jnp.float32)).astype(jnp.bfloat16)
    return high, low


def dot(left, right):
    return jnp.dot(left, right, preferred_element_type=jnp.float32)


def dot_exact(left, right):
    return jnp.dot(
        left, right, preferred_element_type=jnp.float32, precision=lax.Precision.HIGHEST
    )


def harmonic_mean(left, right):
    return 2.0 * left * right / (left + right)


def look_up(region, table_ref):
    found = jnp.full(region.shape, table_ref[0], jnp.float32)
    for index in range(1, REGIONS):
        found = jnp.where(region == float(index), table_ref[index], found)
    return found


def in_groups(block, group):
    return jnp.concatenate([block[group], block[group + GROUPS]], axis=0)


def fill_factors(sigma_ref, cap_ref, region_ref, mask_ref, row_region, col_region, spread, factors):
    lane = lax.broadcasted_iota(jnp.int32, (NZ, LANES), 1)
    first = lane < COLS
    column = jnp.where(first, lane, lane - COLS)
    region = [in_groups(region_ref, g).astype(jnp.float32).T for g in range(GROUPS)]
    conduct = [look_up(r, sigma_ref) for r in region]
    row_halo = look_up(row_region[...].T, sigma_ref)
    is_edge = (column == 0) | (column == COLS - 1)
    col_spread = dot_exact(col_region[...].T, spread)
    below = jnp.where(first, row_halo, pltpu.roll(conduct[GROUPS - 1], COLS, 1))
    above = jnp.where(first, pltpu.roll(conduct[0], COLS, 1), row_halo)
    stack = [below] + conduct + [above]
    faces = [harmonic_mean(stack[g], stack[g + 1]) for g in range(GROUPS + 1)]
    layer = lax.broadcasted_iota(jnp.int32, (NZ, LANES), 0)
    for g in range(GROUPS + 1):
        factors[GX + g] = faces[g]
    for g in range(GROUPS):
        here = conduct[g]
        plus = harmonic_mean(here, pltpu.roll(here, LANES - 1, 1))
        plus = jnp.where(column == COLS - 1, 0.0, plus)
        minus = harmonic_mean(here, pltpu.roll(here, 1, 1))
        minus = jnp.where(column == 0, 0.0, minus)
        outer = col_spread[:, g * LANES : (g + 1) * LANES]
        halo = jnp.where(is_edge, harmonic_mean(here, outer), 0.0)
        upper = harmonic_mean(here, pltpu.roll(here, NZ - 1, 0))
        upper = jnp.where(layer == NZ - 1, 0.0, upper)
        lower = harmonic_mean(here, pltpu.roll(here, 1, 0))
        lower = jnp.where(layer == 0, 0.0, lower)
        diode = in_groups(mask_ref, g).astype(jnp.float32).T
        factors[GYP + g] = plus
        factors[GYM + g] = minus
        factors[GYH + g] = halo
        factors[GZP + g] = upper
        factors[GZM + g] = lower
        factors[CAP + g] = look_up(region[g], cap_ref)
        factors[DIO + g] = diode
        factors[GSUM + g] = (
            faces[g] + faces[g + 1] + plus + minus + halo + upper + lower + 0.5 * diode
        )


def diode_terms(volt, forward, backward):
    high, low = split(volt)
    samples = dot(forward, jnp.concatenate([high, high, low, low], axis=0))
    odd = jnp.tanh(samples)
    even = jnp.abs(samples) - jnp.log(1.0 + jnp.abs(odd))
    spectrum = dot(backward, jnp.concatenate(split(even) + split(odd), axis=0))
    return spectrum[:KC] + spectrum[KC:]


def kernel(
    sigma_ref,
    cap_ref,
    volt_ref,
    drive_ref,
    region_ref,
    mask_ref,
    row_ref,
    col_ref,
    row_region,
    col_region,
    forward_ref,
    backward_ref,
    rates_ref,
    spread_ref,
    out_ref,
    squares_ref,
    turned,
    factors,
):
    step = pl.program_id(0)

    def turn():
        for g in range(GROUPS):
            turned[step, :, g * LANES : (g + 1) * LANES] = in_groups(volt_ref, g).T

    def residual():
        pair = step - 1
        before = jnp.maximum(pair - 1, 0)
        lane = lax.broadcasted_iota(jnp.int32, (KC, LANES), 1)
        first = lane < COLS
        row_halo = row_ref[...].T
        col_halo = dot_exact(col_ref[...].T, spread_ref[...])
        parts = [[] for _ in range(GROUPS)]
        for half in range(2):
            layer = 2 * pair + half
            mine = slice(half * KC, (half + 1) * KC)
            other = slice((1 - half) * KC, (2 - half) * KC)
            diode = diode_terms(turned[pair, mine, :], forward_ref[...], backward_ref[...])

            def factor(index):
                return factors[index, pl.ds(layer, 1), :]

            def group_of(which, rows, g):
                return turned[which, rows, g * LANES : (g + 1) * LANES]

            volts = [group_of(pair, mine, g) for g in range(GROUPS)]
            halo = row_halo[mine]
            below = jnp.where(first, halo, pltpu.roll(volts[GROUPS - 1], COLS, 1))
            above = jnp.where(first, pltpu.roll(volts[0], COLS, 1), halo)
            stack = [below] + volts + [above]
            for g in range(GROUPS):
                here = volts[g]
                down = group_of(before if half == 0 else pair, other, g)
                up = group_of(pair if half == 0 else pair + 1, other, g)
                edge = col_halo[mine, g * LANES : (g + 1) * LANES]
                swapped = jnp.concatenate([here[KC // 2 :], here[: KC // 2]], axis=0)
                total = factor(GSUM + g) * here
                total -= factor(GX + g) * stack[g]
                total -= factor(GX + g + 1) * stack[g + 2]
                total -= factor(GYP + g) * pltpu.roll(here, LANES - 1, 1)
                total -= factor(GYM + g) * pltpu.roll(here, 1, 1)
                total -= factor(GYH + g) * edge
                total -= factor(GZP + g) * up
                total -= factor(GZM + g) * down
                total += factor(CAP + g) * rates_ref[...] * swapped
                total += factor(DIO + g) * diode[:, g * LANES : (g + 1) * LANES]
                parts[g].append(total)
        squares = jnp.zeros((8, LANES), jnp.float32)
        for g in range(GROUPS):
            cells = jnp.concatenate(parts[g], axis=0).T
            for which in range(2):
                row = g + which * GROUPS
                value = cells[which * COLS : (which + 1) * COLS] - drive_ref[row]
                out_ref[row] = value
                squares += jnp.sum((value * value).reshape(COLS // 8, 8, LANES), axis=0)
        squares_ref[...] = jnp.where(step == 1, squares, squares_ref[...] + squares)

    @pl.when(step == 0)
    def _():
        fill_factors(
            sigma_ref, cap_ref, region_ref, mask_ref, row_region, col_region, spread_ref[...], factors
        )
        turn()

    @pl.when(step > 0)
    def _():
        turn()
        residual()


def local_residual(volt, drive, region, mask, rows, cols, sigma_table, cap_table):
    forward, backward, rates, spread = constant_tables()
    width = NZ * KC
    now = lambda s: jnp.minimum(s, PAIRS - 1)
    late = lambda s: jnp.maximum(s - 1, 0)
    whole = lambda *shape: pl.BlockSpec(shape, lambda s: (0,) * len(shape))
    smem = pl.BlockSpec(memory_space=pltpu.SMEM)
    samples = CELLS * NZ * S
    return pl.pallas_call(
        kernel,
        grid=(PAIRS + 1,),
        in_specs=[
            smem,
            smem,
            pl.BlockSpec((ROWS, COLS, LANES), lambda s: (0, 0, now(s))),
            pl.BlockSpec((ROWS, COLS, LANES), lambda s: (0, 0, late(s))),
            whole(ROWS, COLS, NZ),
            whole(ROWS, COLS, NZ),
            pl.BlockSpec((2 * COLS, LANES), lambda s: (0, late(s))),
            pl.BlockSpec((2 * ROWS, LANES), lambda s: (0, late(s))),
            whole(2 * COLS, NZ),
            whole(2 * ROWS, NZ),
            whole(*forward.shape),
            whole(*backward.shape),
            whole(*rates.shape),
            whole(*spread.shape),
        ],
        out_specs=[
            pl.BlockSpec((ROWS, COLS, LANES), lambda s: (0, 0, late(s))),
            whole(8, LANES),
        ],
        out_shape=[
            jax.ShapeDtypeStruct((ROWS, COLS, width), jnp.float32),
            jax.ShapeDtypeStruct((8, LANES), jnp.float32),
        ],
        scratch_shapes=[
            pltpu.VMEM((PAIRS + 1, LANES, CELLS), jnp.float32),
            pltpu.VMEM((FIELDS, NZ, LANES), jnp.float32),
        ],
        compiler_params=pltpu.CompilerParams(
            dimension_semantics=("arbitrary",), vmem_limit_bytes=48 * 1024 * 1024
        ),
        cost_estimate=pl.CostEstimate(
            flops=samples * 1000, bytes_accessed=3 * 4 * CELLS * width, transcendentals=2 * samples
        ),
        name="residual",
    )(
        sigma_table,
        cap_table,
        volt,
        drive,
        region,
        mask,
        rows[0],
        cols[0],
        rows[1],
        cols[1],
        jnp.asarray(forward),
        jnp.asarray(backward),
        jnp.asarray(rates),
        jnp.asarray(spread),
    )


def neighbours(volt, region, axis, dim, periodic):
    count = lax.axis_size(axis)
    forward = [(i, i + 1) for i in range(count - 1)]
    if periodic:
        forward.append((count - 1, 0))
    backward = [(target, source) for source, target in forward]
    extent = volt.shape[dim]

    def slab(index):
        cells = lax.index_in_dim(volt, index, dim, keepdims=False)
        kinds = lax.index_in_dim(region, index, dim, keepdims=False).astype(jnp.float32)
        return jnp.pad(jnp.concatenate([cells, kinds + 1.0], axis=1), ((0, 0), (0, LANES - NZ)))

    low = lax.ppermute(slab(extent - 1), axis, forward)
    high = lax.ppermute(slab(0), axis, backward)
    both = jnp.concatenate([low, high], axis=0)
    width = NZ * KC
    return both[:, :width], both[:, width : width + NZ]


def body(volt, drive, region, diode_mask, sigma_table, cap_table):
    row_volt, row_kind = neighbours(volt, region, "gx", 0, True)
    col_volt, col_kind = neighbours(volt, region, "gy", 1, False)
    kinds = jnp.arange(1, REGIONS + 1, dtype=jnp.float32)
    col_conduct = jnp.sum(
        jnp.where(col_kind[..., None] == kinds, sigma_table, 0.0), axis=-1
    )
    residual, squares = local_residual(
        volt,
        drive,
        region,
        diode_mask,
        (row_volt, row_kind - 1.0),
        (col_volt, col_conduct),
        sigma_table,
        cap_table,
    )
    partial = jnp.sum(squares.reshape(8, 2, KC), axis=(0, 1))
    summed = lax.psum(partial, ("gx", "gy"))
    cells_total = CELLS * NZ * lax.axis_size("gx") * lax.axis_size("gy")
    return residual, jnp.sqrt(summed / cells_total + norm_eps)


def solution(mesh):
    spec = P("gx", "gy", None)
    return jax.shard_map(
        body,
        mesh=mesh,
        in_specs=(spec, spec, spec, spec, P(), P()),
        out_specs=(spec, P()),
        check_vma=False,
    )
```

```python
import functools
import math

import jax
import jax.numpy as jnp
import numpy as np
from jax import lax
from jax.experimental import pallas as pl
from jax.experimental.pallas import tpu as pltpu
from jax.sharding import PartitionSpec as P

NZ = 32
H = 32
KC = 64
S = 256
REGIONS = 8
ROWS = 8
COLS = 64
PAIRS = NZ // 2
LANES = 128
GROUPS = ROWS * COLS // LANES
CELLS = ROWS * COLS
WIDTH = NZ * KC

base_freq = 0.1
norm_eps = 1e-06

GX = 0
GYP = GX + GROUPS + 1
GYM = GYP + GROUPS
GZP = GYM + GROUPS
GZM = GZP + GROUPS
CAP = GZM + GROUPS
DIO = CAP + GROUPS
GSUM = DIO + GROUPS
FIELDS = GSUM + GROUPS

CHUNK = 64


def halves(table):
    high = table.astype(jnp.bfloat16)
    low = (table - high.astype(np.float64)).astype(jnp.bfloat16)
    return high, low


def constant_tables():
    orders = np.arange(1, H + 1, dtype=np.float64)
    angles = orders[:, None] * (2.0 * math.pi * np.arange(S) / S)[None, :]
    cosines, sines = np.cos(angles), np.sin(angles)
    synthesis = np.concatenate([cosines, sines], axis=0)
    high, low = halves(synthesis.T)
    forward = np.concatenate([high, low, high, low], axis=1)
    scaled = base_freq * orders[:, None]
    from_even = halves(synthesis / S)
    from_odd = halves(np.concatenate([scaled * sines, -scaled * cosines], axis=0) / S)
    rows = []
    for part in range(2):
        blocks = []
        for first in range(0, S, CHUNK):
            even = from_even[part][:, first : first + CHUNK]
            odd = from_odd[part][:, first : first + CHUNK]
            blocks += [even, even, odd, odd]
        rows.append(np.concatenate(blocks, axis=1))
    backward = np.concatenate(rows, axis=0).astype(np.float32)
    rates = np.concatenate([scaled, -scaled], axis=0).astype(np.float32)
    rates = np.ascontiguousarray(np.broadcast_to(rates, (KC, LANES)))
    spread = np.zeros((2 * ROWS, CELLS), np.float32)
    for row in range(ROWS):
        group, half = row % GROUPS, row // GROUPS
        spread[row, group * LANES + half * COLS] = 1.0
        spread[ROWS + row, group * LANES + half * COLS + COLS - 1] = 1.0
    widen = np.tile(np.repeat(np.eye(NZ), KC, axis=1), (3, 1)).astype(jnp.bfloat16)
    return forward, backward, rates, spread, widen


def split(values):
    high = values.astype(jnp.bfloat16)
    low = (values - high.astype(jnp.float32)).astype(jnp.bfloat16)
    return high, low


def dot(left, right):
    return jnp.dot(left, right, preferred_element_type=jnp.float32)


def dot_exact(left, right):
    return jnp.dot(
        left, right, preferred_element_type=jnp.float32, precision=lax.Precision.HIGHEST
    )


def harmonic_mean(left, right):
    return 2.0 * left * right / (left + right)


def look_up(region, table_ref):
    found = jnp.zeros(region.shape, jnp.float32)
    for index in range(REGIONS):
        found = jnp.where(region == float(index), table_ref[index], found)
    return found


def in_groups(block, group):
    return jnp.concatenate([block[group], block[group + GROUPS]], axis=0)


def layers_of(ref, pair):
    lanes = pl.ds(pl.multiple_of(pair * LANES, LANES), LANES)
    return ref.at[..., lanes]


def group_lanes(g):
    return slice(g * LANES, (g + 1) * LANES)


def diode_terms(volt, forward, backward):
    high, low = split(volt)
    samples = dot(forward, jnp.concatenate([high, high, low, low], axis=0))
    blocks = []
    for first in range(0, S, CHUNK):
        sample = samples[first : first + CHUNK]
        odd = jnp.tanh(sample)
        even = jnp.abs(sample) - jnp.log(1.0 + jnp.abs(odd))
        coarse = jnp.round(even)
        near = odd.astype(jnp.bfloat16).astype(jnp.float32)
        blocks += [coarse, even - coarse, near, odd - near]
    spectrum = dot(backward, jnp.concatenate(blocks, axis=0))
    return spectrum[:KC] + spectrum[KC:]


def diode_kernel(volt_ref, forward_ref, backward_ref, turned, diode_ref):
    def turn(pair):
        block = layers_of(volt_ref, pair)
        for g in range(GROUPS):
            turned[pair, :, group_lanes(g)] = in_groups(block, g).T

    def at_pair(pair):
        for half in range(2):
            mine = slice(half * KC, (half + 1) * KC)
            diode_ref[pair, mine, :] = diode_terms(
                turned[pair, mine, :], forward_ref[...], backward_ref[...]
            )

    turn(0)

    @pl.loop(0, PAIRS)
    def _(pair):
        at_pair(pair)
        turn(jnp.minimum(pair + 1, PAIRS - 1))


def beside(block, group):
    return jnp.concatenate([block[group], block[group + GROUPS]], axis=1).astype(jnp.float32)


def kinds_of(message):
    return message[:, WIDTH : WIDTH + NZ] - 1.0


def fill_factors(sigma_ref, cap_ref, region_ref, mask_ref, rows, cols, own_cols, spread, factors):
    lane = lax.broadcasted_iota(jnp.int32, (NZ, LANES), 1)
    first = lane < COLS
    column = jnp.where(first, lane, lane - COLS)
    region = [beside(region_ref, g) for g in range(GROUPS)]
    conduct = [look_up(r, sigma_ref) for r in region]
    row_kinds = jnp.concatenate([message[:, WIDTH:] for message in rows], axis=0).T
    row_halo = look_up(row_kinds[:NZ] - 1.0, sigma_ref)
    outer = look_up(jnp.concatenate([kinds_of(m) for m in cols], axis=0), sigma_ref)
    inner = look_up(jnp.concatenate([kinds_of(m) for m in own_cols], axis=0), sigma_ref)
    rim = harmonic_mean(inner, outer)
    rim_spread = dot_exact(rim.T, spread)
    below = jnp.where(first, row_halo, pltpu.roll(conduct[GROUPS - 1], COLS, 1))
    above = jnp.where(first, pltpu.roll(conduct[0], COLS, 1), row_halo)
    stack = [below] + conduct + [above]
    faces = [harmonic_mean(stack[g], stack[g + 1]) for g in range(GROUPS + 1)]
    layer = lax.broadcasted_iota(jnp.int32, (NZ, LANES), 0)
    for g in range(GROUPS + 1):
        factors[GX + g] = faces[g]
    for g in range(GROUPS):
        here = conduct[g]
        plus = harmonic_mean(here, pltpu.roll(here, LANES - 1, 1))
        plus = jnp.where(column == COLS - 1, 0.0, plus)
        minus = jnp.where(column == 0, 0.0, harmonic_mean(here, pltpu.roll(here, 1, 1)))
        upper = harmonic_mean(here, pltpu.roll(here, NZ - 1, 0))
        upper = jnp.where(layer == NZ - 1, 0.0, upper)
        lower = jnp.where(layer == 0, 0.0, harmonic_mean(here, pltpu.roll(here, 1, 0)))
        diode = beside(mask_ref, g)
        factors[GYP + g] = plus
        factors[GYM + g] = minus
        factors[GZP + g] = upper
        factors[GZM + g] = lower
        factors[CAP + g] = look_up(region[g], cap_ref)
        factors[DIO + g] = diode
        factors[GSUM + g] = (
            faces[g] + faces[g + 1] + plus + minus + rim_spread[:, group_lanes(g)]
            + upper + lower + 0.5 * diode
        )
    return rim


def residual_kernel(
    sigma_ref,
    cap_ref,
    turned,
    diode_ref,
    drive_ref,
    region_ref,
    mask_ref,
    row_low,
    row_high,
    col_low,
    col_high,
    own_first,
    own_last,
    rates_ref,
    spread_ref,
    widen_ref,
    out_ref,
    squares_ref,
    factors,
    rim_flux,
    sums,
):
    cols = [col_low[...], col_high[...]]
    rim = fill_factors(
        sigma_ref,
        cap_ref,
        region_ref,
        mask_ref,
        [row_low, row_high],
        cols,
        [own_first[...], own_last[...]],
        spread_ref[...],
        factors,
    )
    top = rim.astype(jnp.bfloat16).astype(jnp.float32)
    middle = (rim - top).astype(jnp.bfloat16).astype(jnp.float32)
    rim = jnp.concatenate([top, middle, rim - top - middle], axis=1).astype(jnp.bfloat16)
    rim_flux[...] = dot(rim, widen_ref[...]) * jnp.concatenate([c[:, :WIDTH] for c in cols], axis=0)
    first = lax.broadcasted_iota(jnp.int32, (KC, LANES), 1) < COLS
    at_low = lax.broadcasted_iota(jnp.int32, (8, LANES), 0) == 0
    at_high = lax.broadcasted_iota(jnp.int32, (8, LANES), 0) == 7

    def gather(pair):
        row_halo = jnp.concatenate(
            [layers_of(row_low, pair)[...], layers_of(row_high, pair)[...]], axis=0
        ).T
        for half in range(2):
            layer = 2 * pair + half
            mine = slice(half * KC, (half + 1) * KC)
            other = slice((1 - half) * KC, (2 - half) * KC)
            before = jnp.maximum(pair - 1, 0) if half == 0 else pair
            after = pair if half == 0 else jnp.minimum(pair + 1, PAIRS - 1)

            def factor(index):
                return factors[index, pl.ds(layer, 1), :]

            volts = [turned[pair, mine, group_lanes(g)] for g in range(GROUPS)]
            halo = row_halo[mine]
            below = jnp.where(first, halo, pltpu.roll(volts[GROUPS - 1], COLS, 1))
            above = jnp.where(first, pltpu.roll(volts[0], COLS, 1), halo)
            stack = [below] + volts + [above]
            for g in range(GROUPS):
                here = volts[g]
                swapped = jnp.concatenate([here[KC // 2 :], here[: KC // 2]], axis=0)
                total = factor(GSUM + g) * here
                total -= factor(GX + g) * stack[g]
                total -= factor(GX + g + 1) * stack[g + 2]
                total -= factor(GYP + g) * pltpu.roll(here, LANES - 1, 1)
                total -= factor(GYM + g) * pltpu.roll(here, 1, 1)
                total -= factor(GZP + g) * turned[after, other, group_lanes(g)]
                total -= factor(GZM + g) * turned[before, other, group_lanes(g)]
                total += factor(CAP + g) * rates_ref[...] * swapped
                total += factor(DIO + g) * diode_ref[pair, mine, group_lanes(g)]
                sums[mine, group_lanes(g)] = total

    def finish(pair, squares):
        drive = layers_of(drive_ref, pair)
        out = layers_of(out_ref, pair)
        edges = layers_of(rim_flux, pair)
        for g in range(GROUPS):
            cells = sums[:, group_lanes(g)].T
            for which in range(2):
                row = g + which * GROUPS
                value = cells[which * COLS : (which + 1) * COLS] - drive[row]
                low = jnp.where(at_low, edges[row : row + 1, :], 0.0)
                high = jnp.where(at_high, edges[ROWS + row : ROWS + row + 1, :], 0.0)
                value = jnp.concatenate(
                    [value[:8] - low, value[8 : COLS - 8], value[COLS - 8 :] - high], axis=0
                )
                out[row] = value
                squares += jnp.sum((value * value).reshape(COLS // 8, 8, LANES), axis=0)
        return squares

    gather(0)

    def step(pair, squares):
        squares = finish(pair - 1, squares)
        gather(pair)
        return squares

    squares = lax.fori_loop(1, PAIRS, step, jnp.zeros((8, LANES), jnp.float32))
    squares = jnp.sum(finish(PAIRS - 1, squares), axis=0, keepdims=True)
    squares += pltpu.roll(squares, KC, 1)
    squares_ref[...] = jnp.broadcast_to(squares, squares_ref.shape)


def in_vmem(count):
    return [pl.BlockSpec(memory_space=pltpu.VMEM)] * count


def pack_kernel(volt_ref, region_ref, row_first, row_last, col_first, col_last):
    kinds = [region_ref[row].astype(jnp.float32).T + 1.0 for row in range(ROWS)]

    def put(message, volts, regions):
        message[:, :WIDTH] = volts
        padding = jnp.zeros((regions.shape[0], LANES - NZ), jnp.float32)
        message[:, WIDTH:] = jnp.concatenate([regions, padding], axis=1)

    put(row_first, volt_ref[0], kinds[0])
    put(row_last, volt_ref[ROWS - 1], kinds[ROWS - 1])
    for message, col in ((col_first, 0), (col_last, COLS - 1)):
        regions = jnp.concatenate([kind[col : col + 1] for kind in kinds], axis=0)
        put(message, volt_ref[:, col, :], regions)


def packed(volt, region):
    shapes = [(COLS, WIDTH + LANES)] * 2 + [(ROWS, WIDTH + LANES)] * 2
    return pl.pallas_call(
        pack_kernel,
        in_specs=in_vmem(2),
        out_specs=in_vmem(4),
        out_shape=[jax.ShapeDtypeStruct(shape, jnp.float32) for shape in shapes],
        compiler_params=pltpu.CompilerParams(vmem_limit_bytes=8 * 1024 * 1024),
        name="pack",
    )(volt, region)


def diode_part(volt):
    forward, backward = constant_tables()[:2]
    samples = CELLS * NZ * S
    whole = jax.ShapeDtypeStruct((PAIRS, LANES, CELLS), jnp.float32)
    return pl.pallas_call(
        diode_kernel,
        in_specs=in_vmem(3),
        out_specs=in_vmem(2),
        out_shape=[whole, whole],
        compiler_params=pltpu.CompilerParams(vmem_limit_bytes=16 * 1024 * 1024),
        cost_estimate=pl.CostEstimate(
            flops=samples * 1000, bytes_accessed=4 * CELLS * WIDTH, transcendentals=2 * samples
        ),
        name="diode",
    )(volt, jnp.asarray(forward), jnp.asarray(backward))


def whole_residual(turned, diode, drive, region, mask, halos, own_cols, tables, copies):
    rates, spread, widen = constant_tables()[2:]
    smem = pl.BlockSpec(memory_space=pltpu.SMEM)
    return pl.pallas_call(
        residual_kernel,
        in_specs=[smem, smem] + in_vmem(14),
        out_specs=in_vmem(2),
        out_shape=[
            jax.ShapeDtypeStruct((ROWS, COLS, WIDTH), jnp.float32),
            jax.ShapeDtypeStruct((copies, LANES), jnp.float32),
        ],
        scratch_shapes=[
            pltpu.VMEM((FIELDS, NZ, LANES), jnp.float32),
            pltpu.VMEM((2 * ROWS, WIDTH), jnp.float32),
            pltpu.VMEM((LANES, CELLS), jnp.float32),
        ],
        compiler_params=pltpu.CompilerParams(vmem_limit_bytes=16 * 1024 * 1024),
        cost_estimate=pl.CostEstimate(
            flops=30 * CELLS * WIDTH, bytes_accessed=2 * 4 * CELLS * WIDTH, transcendentals=0
        ),
        name="residual",
    )(
        *tables,
        turned,
        diode,
        drive,
        region,
        mask,
        *halos,
        *own_cols,
        jnp.asarray(rates),
        jnp.asarray(spread),
        jnp.asarray(widen),
    )


def neighbours(first, last, axis, periodic):
    count = lax.axis_size(axis)
    forward = [(i, i + 1) for i in range(count - 1)]
    if periodic:
        forward.append((count - 1, 0))
    backward = [(target, source) for source, target in forward]
    return lax.ppermute(last, axis, forward), lax.ppermute(first, axis, backward)


def exchanged_sum(copies, axis):
    return jnp.sum(lax.all_to_all(copies, axis, 0, 0, tiled=True), axis=0)


def body(volt, drive, region, diode_mask, sigma_table, cap_table):
    by_layer = jnp.transpose(region, (0, 2, 1))
    mask = jnp.transpose(diode_mask, (0, 2, 1))
    row_first, row_last, col_first, col_last = packed(volt, by_layer)
    rows = neighbours(row_first, row_last, "gx", True)
    cols = neighbours(col_first, col_last, "gy", False)
    turned, diode = diode_part(volt)
    nx, ny = lax.axis_size("gx"), lax.axis_size("gy")
    residual, squares = whole_residual(
        turned,
        diode,
        drive,
        by_layer,
        mask,
        rows + cols,
        (col_first, col_last),
        (sigma_table, cap_table),
        nx,
    )
    over_x = exchanged_sum(squares, "gx")
    summed = exchanged_sum(jnp.broadcast_to(over_x, (ny, LANES)), "gy")[:KC]
    return residual, jnp.sqrt(summed / (CELLS * NZ * nx * ny) + norm_eps)


def solution(mesh):
    spec = P("gx", "gy", None)
    return jax.shard_map(
        body,
        mesh=mesh,
        in_specs=(spec, spec, spec, spec, P(), P()),
        out_specs=(spec, P()),
        check_vma=False,
    )
```

```python
import functools
import math

import jax
import jax.numpy as jnp
import numpy as np
from jax import lax
from jax.experimental import pallas as pl
from jax.experimental.pallas import tpu as pltpu
from jax.sharding import PartitionSpec as P

NZ = 32
H = 32
KC = 64
S = 256
REGIONS = 8
ROWS = 8
COLS = 64
PAIRS = NZ // 2
LANES = 128
GROUPS = ROWS * COLS // LANES
CELLS = ROWS * COLS
WIDTH = NZ * KC

base_freq = 0.1
norm_eps = 1e-06

GX = 0
GYP = GX + GROUPS + 1
GYM = GYP + GROUPS
GZP = GYM + GROUPS
GZM = GZP + GROUPS
CAP = GZM + GROUPS
DIO = CAP + GROUPS
GSUM = DIO + GROUPS
FIELDS = GSUM + GROUPS

UNROLL = 2
PACK_MIB = 46

CHUNK = 64


def halves(table):
    high = table.astype(jnp.bfloat16)
    low = (table - high.astype(np.float64)).astype(jnp.bfloat16)
    return high, low


def constant_tables():
    orders = np.arange(1, H + 1, dtype=np.float64)
    angles = orders[:, None] * (2.0 * math.pi * np.arange(S) / S)[None, :]
    cosines, sines = np.cos(angles), np.sin(angles)
    synthesis = np.concatenate([cosines, sines], axis=0)
    high, low = halves(synthesis.T)
    forward = np.concatenate([high, low, high, low], axis=1)
    scaled = base_freq * orders[:, None]
    from_even = halves(synthesis / S)
    from_odd = halves(np.concatenate([scaled * sines, -scaled * cosines], axis=0) / S)
    rows = []
    for part in range(2):
        blocks = []
        for first in range(0, S, CHUNK):
            even = from_even[part][:, first : first + CHUNK]
            odd = from_odd[part][:, first : first + CHUNK]
            blocks += [even, even, odd, odd]
        rows.append(np.concatenate(blocks, axis=1))
    backward = np.concatenate(rows, axis=0).astype(np.float32)
    rates = np.concatenate([scaled, -scaled], axis=0).astype(np.float32)
    rates = np.ascontiguousarray(np.broadcast_to(rates, (KC, LANES)))
    spread = np.zeros((2 * ROWS, CELLS), np.float32)
    for row in range(ROWS):
        group, half = row % GROUPS, row // GROUPS
        spread[row, group * LANES + half * COLS] = 1.0
        spread[ROWS + row, group * LANES + half * COLS + COLS - 1] = 1.0
    widen = np.tile(np.repeat(np.eye(NZ), KC, axis=1), (3, 1)).astype(jnp.bfloat16)
    return forward, backward, rates, spread, widen


def split(values):
    high = values.astype(jnp.bfloat16)
    low = (values - high.astype(jnp.float32)).astype(jnp.bfloat16)
    return high, low


def dot(left, right):
    return jnp.dot(left, right, preferred_element_type=jnp.float32)


def dot_exact(left, right):
    return jnp.dot(
        left, right, preferred_element_type=jnp.float32, precision=lax.Precision.HIGHEST
    )


def harmonic_mean(left, right):
    return 2.0 * left * right / (left + right)


def look_up(region, table_ref):
    found = jnp.zeros(region.shape, jnp.float32)
    for index in range(REGIONS):
        found = jnp.where(region == float(index), table_ref[index], found)
    return found


def in_groups(block, group):
    return jnp.concatenate([block[group], block[group + GROUPS]], axis=0)


def layers_of(ref, pair):
    lanes = pl.ds(pl.multiple_of(pair * LANES, LANES), LANES)
    return ref.at[..., lanes]


def group_lanes(g):
    return slice(g * LANES, (g + 1) * LANES)


def sampled(volt, forward):
    high, low = split(volt)
    return dot(forward, jnp.concatenate([high, high, low, low], axis=0))


def bend(samples, bent):
    for first in range(0, S, CHUNK):
        sample = samples[first : first + CHUNK]
        odd = jnp.tanh(sample)
        even = jnp.abs(sample) - jnp.log(1.0 + jnp.abs(odd))
        coarse = jnp.round(even)
        near = odd.astype(jnp.bfloat16).astype(jnp.float32)
        for index, term in enumerate((coarse, even - coarse, near, odd - near)):
            row = 4 * first + index * CHUNK
            bent[row : row + CHUNK] = term


def diode_kernel(volt_ref, forward_ref, backward_ref, turned, diode_ref, *scratch):
    samples, bents = scratch[:2], scratch[2:]

    def turn(pair):
        block = layers_of(volt_ref, pair)
        for g in range(GROUPS):
            turned[pair, :, group_lanes(g)] = in_groups(block, g).T

    def sample(pair, half):
        mine = slice(half * KC, (half + 1) * KC)
        samples[half][...] = sampled(turned[pair, mine, :], forward_ref[...])

    def project(pair, half):
        mine = slice(half * KC, (half + 1) * KC)
        spectrum = dot(backward_ref[...], bents[half][...])
        diode_ref[pair, mine, :] = spectrum[:KC] + spectrum[KC:]

    turn(0)
    turn(1)
    sample(0, 0)
    bents[1][...] = jnp.zeros(bents[1].shape, jnp.float32)

    def at_pair(pair):
        sample(pair, 1)
        project(jnp.maximum(pair - 1, 0), 1)
        bend(samples[0], bents[0])
        sample(jnp.minimum(pair + 1, PAIRS - 1), 0)
        bend(samples[1], bents[1])
        project(pair, 0)
        turn(jnp.minimum(pair + 2, PAIRS - 1))

    @pl.loop(0, PAIRS // UNROLL)
    def _(block):
        for index in range(UNROLL):
            at_pair(UNROLL * block + index)

    project(PAIRS - 1, 1)


def beside(block, group):
    return jnp.concatenate([block[group], block[group + GROUPS]], axis=1).astype(jnp.float32)


def kinds_of(message):
    return message[:, WIDTH : WIDTH + NZ] - 1.0


def fill_factors(sigma_ref, cap_ref, region_ref, mask_ref, rows, cols, own_cols, spread, factors):
    lane = lax.broadcasted_iota(jnp.int32, (NZ, LANES), 1)
    first = lane < COLS
    column = jnp.where(first, lane, lane - COLS)
    region = [beside(region_ref, g) for g in range(GROUPS)]
    conduct = [look_up(r, sigma_ref) for r in region]
    row_kinds = jnp.concatenate([message[:, WIDTH:] for message in rows], axis=0).T
    row_halo = look_up(row_kinds[:NZ] - 1.0, sigma_ref)
    outer = look_up(jnp.concatenate([kinds_of(m) for m in cols], axis=0), sigma_ref)
    inner = look_up(jnp.concatenate([kinds_of(m) for m in own_cols], axis=0), sigma_ref)
    rim = harmonic_mean(inner, outer)
    rim_spread = dot_exact(rim.T, spread)
    below = jnp.where(first, row_halo, pltpu.roll(conduct[GROUPS - 1], COLS, 1))
    above = jnp.where(first, pltpu.roll(conduct[0], COLS, 1), row_halo)
    stack = [below] + conduct + [above]
    faces = [harmonic_mean(stack[g], stack[g + 1]) for g in range(GROUPS + 1)]
    layer = lax.broadcasted_iota(jnp.int32, (NZ, LANES), 0)
    for g in range(GROUPS + 1):
        factors[GX + g] = faces[g]
    for g in range(GROUPS):
        here = conduct[g]
        plus = harmonic_mean(here, pltpu.roll(here, LANES - 1, 1))
        plus = jnp.where(column == COLS - 1, 0.0, plus)
        minus = jnp.where(column == 0, 0.0, harmonic_mean(here, pltpu.roll(here, 1, 1)))
        upper = harmonic_mean(here, pltpu.roll(here, NZ - 1, 0))
        upper = jnp.where(layer == NZ - 1, 0.0, upper)
        lower = jnp.where(layer == 0, 0.0, harmonic_mean(here, pltpu.roll(here, 1, 0)))
        diode = beside(mask_ref, g)
        factors[GYP + g] = plus
        factors[GYM + g] = minus
        factors[GZP + g] = upper
        factors[GZM + g] = lower
        factors[CAP + g] = look_up(region[g], cap_ref)
        factors[DIO + g] = diode
        factors[GSUM + g] = (
            faces[g] + faces[g + 1] + plus + minus + rim_spread[:, group_lanes(g)]
            + upper + lower + 0.5 * diode
        )
    return rim


def residual_kernel(
    sigma_ref,
    cap_ref,
    turned,
    diode_ref,
    drive_ref,
    region_ref,
    mask_ref,
    row_low,
    row_high,
    col_low,
    col_high,
    own_first,
    own_last,
    rates_ref,
    spread_ref,
    widen_ref,
    out_ref,
    squares_ref,
    factors,
    rim_flux,
    *scratch,
):
    sums, ready, sent = scratch[:2], scratch[2], scratch[3]
    cols = [col_low[...], col_high[...]]
    rim = fill_factors(
        sigma_ref,
        cap_ref,
        region_ref,
        mask_ref,
        [row_low, row_high],
        cols,
        [own_first[...], own_last[...]],
        spread_ref[...],
        factors,
    )
    top = rim.astype(jnp.bfloat16).astype(jnp.float32)
    middle = (rim - top).astype(jnp.bfloat16).astype(jnp.float32)
    rim = jnp.concatenate([top, middle, rim - top - middle], axis=1).astype(jnp.bfloat16)
    rim_flux[...] = dot(rim, widen_ref[...]) * jnp.concatenate([c[:, :WIDTH] for c in cols], axis=0)
    first = lax.broadcasted_iota(jnp.int32, (KC, LANES), 1) < COLS
    at_low = lax.broadcasted_iota(jnp.int32, (8, LANES), 0) == 0
    at_high = lax.broadcasted_iota(jnp.int32, (8, LANES), 0) == 7

    def gather(pair, slot):
        row_halo = jnp.concatenate(
            [layers_of(row_low, pair)[...], layers_of(row_high, pair)[...]], axis=0
        ).T
        for half in range(2):
            layer = 2 * pair + half
            mine = slice(half * KC, (half + 1) * KC)
            other = slice((1 - half) * KC, (2 - half) * KC)
            before = jnp.maximum(pair - 1, 0) if half == 0 else pair
            after = pair if half == 0 else jnp.minimum(pair + 1, PAIRS - 1)

            def factor(index):
                return factors[index, pl.ds(layer, 1), :]

            volts = [turned[pair, mine, group_lanes(g)] for g in range(GROUPS)]
            halo = row_halo[mine]
            below = jnp.where(first, halo, pltpu.roll(volts[GROUPS - 1], COLS, 1))
            above = jnp.where(first, pltpu.roll(volts[0], COLS, 1), halo)
            stack = [below] + volts + [above]
            for g in range(GROUPS):
                here = volts[g]
                swapped = jnp.concatenate([here[KC // 2 :], here[: KC // 2]], axis=0)
                total = factor(GSUM + g) * here
                total -= factor(GX + g) * stack[g]
                total -= factor(GX + g + 1) * stack[g + 2]
                total -= factor(GYP + g) * pltpu.roll(here, LANES - 1, 1)
                total -= factor(GYM + g) * pltpu.roll(here, 1, 1)
                total -= factor(GZP + g) * turned[after, other, group_lanes(g)]
                total -= factor(GZM + g) * turned[before, other, group_lanes(g)]
                total += factor(CAP + g) * rates_ref[...] * swapped
                total += factor(DIO + g) * diode_ref[pair, mine, group_lanes(g)]
                sums[slot][mine, group_lanes(g)] = total

    def copy_out(pair):
        return pltpu.make_async_copy(ready.at[pair], layers_of(out_ref, pair), sent.at[pair])

    def finish(pair, slot, squares):
        drive = layers_of(drive_ref, pair)
        edges = layers_of(rim_flux, pair)
        for g in range(GROUPS):
            cells = sums[slot][:, group_lanes(g)].T
            for which in range(2):
                row = g + which * GROUPS
                value = cells[which * COLS : (which + 1) * COLS] - drive[row]
                low = jnp.where(at_low, edges[row : row + 1, :], 0.0)
                high = jnp.where(at_high, edges[ROWS + row : ROWS + row + 1, :], 0.0)
                value = jnp.concatenate(
                    [value[:8] - low, value[8 : COLS - 8], value[COLS - 8 :] - high], axis=0
                )
                ready[pair, row] = value
                squares += jnp.sum((value * value).reshape(COLS // 8, 8, LANES), axis=0)
        return squares

    for slot in range(2):
        gather(slot, slot)

    def step(index, squares):
        pair = 2 * index
        for slot in range(2):
            squares = finish(pair - 2 + slot, slot, squares)
            gather(pair + slot, slot)
        for slot in range(2):
            copy_out(pair - 2 + slot).start()
        return squares

    squares = lax.fori_loop(1, PAIRS // 2, step, jnp.zeros((8, LANES), jnp.float32))
    for slot in range(2):
        squares = finish(PAIRS - 2 + slot, slot, squares)
        copy_out(PAIRS - 2 + slot).start()
    squares = jnp.sum(squares, axis=0, keepdims=True)
    squares += pltpu.roll(squares, KC, 1)
    squares_ref[...] = jnp.broadcast_to(squares, squares_ref.shape)
    for pair in range(PAIRS):
        copy_out(pair).wait()


def in_vmem(count):
    return [pl.BlockSpec(memory_space=pltpu.VMEM)] * count


def pack_kernel(volt_hbm, region_hbm, *refs):
    row_first, row_last, col_first, col_last, volt_ref, region_ref, arrived = refs
    fetches = [
        pltpu.make_async_copy(volt_hbm.at[row], volt_ref.at[row], arrived.at[row])
        for row in range(ROWS)
    ]
    fetches.append(pltpu.make_async_copy(region_hbm, region_ref, arrived.at[ROWS]))
    for fetch in reversed(fetches):
        fetch.start()
    fetches[ROWS].wait()
    kinds = [region_ref[row].astype(jnp.float32).T + 1.0 for row in range(ROWS)]

    def put(message, volts, regions):
        message[:, :WIDTH] = volts
        padding = jnp.zeros((regions.shape[0], LANES - NZ), jnp.float32)
        message[:, WIDTH:] = jnp.concatenate([regions, padding], axis=1)

    for row in reversed(range(ROWS)):
        fetches[row].wait()
    put(row_last, volt_ref[ROWS - 1], kinds[ROWS - 1])
    put(row_first, volt_ref[0], kinds[0])
    for message, col in ((col_first, 0), (col_last, COLS - 1)):
        regions = jnp.concatenate([kind[col : col + 1] for kind in kinds], axis=0)
        put(message, volt_ref[:, col, :], regions)


def packed(volt, region):
    shapes = [(COLS, WIDTH + LANES)] * 2 + [(ROWS, WIDTH + LANES)] * 2 + [volt.shape]
    return pl.pallas_call(
        pack_kernel,
        in_specs=[pl.BlockSpec(memory_space=pltpu.HBM)] * 2,
        out_specs=in_vmem(5),
        out_shape=[jax.ShapeDtypeStruct(shape, jnp.float32) for shape in shapes],
        scratch_shapes=[
            pltpu.VMEM(region.shape, region.dtype),
            pltpu.SemaphoreType.DMA((ROWS + 1,)),
        ],
        compiler_params=pltpu.CompilerParams(vmem_limit_bytes=PACK_MIB * 1024 * 1024),
        name="pack",
    )(volt, region)


def diode_part(volt):
    forward, backward = constant_tables()[:2]
    samples = CELLS * NZ * S
    whole = jax.ShapeDtypeStruct((PAIRS, LANES, CELLS), jnp.float32)
    return pl.pallas_call(
        diode_kernel,
        in_specs=in_vmem(3),
        out_specs=in_vmem(2),
        out_shape=[whole, whole],
        scratch_shapes=[pltpu.VMEM((S, CELLS), jnp.float32)] * 2
        + [pltpu.VMEM((4 * S, CELLS), jnp.float32)] * 2,
        compiler_params=pltpu.CompilerParams(vmem_limit_bytes=16 * 1024 * 1024),
        cost_estimate=pl.CostEstimate(
            flops=samples * 1000, bytes_accessed=4 * CELLS * WIDTH, transcendentals=2 * samples
        ),
        name="diode",
    )(volt, jnp.asarray(forward), jnp.asarray(backward))


def whole_residual(turned, diode, drive, region, mask, halos, own_cols, tables, copies):
    rates, spread, widen = constant_tables()[2:]
    smem = pl.BlockSpec(memory_space=pltpu.SMEM)
    return pl.pallas_call(
        residual_kernel,
        in_specs=[smem, smem] + in_vmem(14),
        out_specs=[pl.BlockSpec(memory_space=pltpu.HBM)] + in_vmem(1),
        out_shape=[
            jax.ShapeDtypeStruct((ROWS, COLS, WIDTH), jnp.float32),
            jax.ShapeDtypeStruct((copies, LANES), jnp.float32),
        ],
        scratch_shapes=[
            pltpu.VMEM((FIELDS, NZ, LANES), jnp.float32),
            pltpu.VMEM((2 * ROWS, WIDTH), jnp.float32),
            pltpu.VMEM((LANES, CELLS), jnp.float32),
            pltpu.VMEM((LANES, CELLS), jnp.float32),
            pltpu.VMEM((PAIRS, ROWS, COLS, LANES), jnp.float32),
            pltpu.SemaphoreType.DMA((PAIRS,)),
        ],
        compiler_params=pltpu.CompilerParams(vmem_limit_bytes=16 * 1024 * 1024),
        cost_estimate=pl.CostEstimate(
            flops=30 * CELLS * WIDTH, bytes_accessed=2 * 4 * CELLS * WIDTH, transcendentals=0
        ),
        name="residual",
    )(
        *tables,
        turned,
        diode,
        drive,
        region,
        mask,
        *halos,
        *own_cols,
        jnp.asarray(rates),
        jnp.asarray(spread),
        jnp.asarray(widen),
    )


def neighbours(first, last, axis, periodic):
    count = lax.axis_size(axis)
    forward = [(i, i + 1) for i in range(count - 1)]
    if periodic:
        forward.append((count - 1, 0))
    backward = [(target, source) for source, target in forward]
    return lax.ppermute(last, axis, forward), lax.ppermute(first, axis, backward)


def exchanged_sum(copies, axis):
    return jnp.sum(lax.all_to_all(copies, axis, 0, 0, tiled=True), axis=0)


def body(volt, drive, region, diode_mask, sigma_table, cap_table):
    by_layer = jnp.transpose(region, (0, 2, 1))
    mask = jnp.transpose(diode_mask, (0, 2, 1))
    row_first, row_last, col_first, col_last, volt = packed(volt, by_layer)
    rows = neighbours(row_first, row_last, "gx", True)
    cols = neighbours(col_first, col_last, "gy", False)
    turned, diode = diode_part(volt)
    nx, ny = lax.axis_size("gx"), lax.axis_size("gy")
    residual, squares = whole_residual(
        turned,
        diode,
        drive,
        by_layer,
        mask,
        rows + cols,
        (col_first, col_last),
        (sigma_table, cap_table),
        nx,
    )
    over_x = exchanged_sum(squares, "gx")
    summed = exchanged_sum(jnp.broadcast_to(over_x, (ny, LANES)), "gy")[:KC]
    return residual, jnp.sqrt(summed / (CELLS * NZ * nx * ny) + norm_eps)


def solution(mesh):
    spec = P("gx", "gy", None)
    return jax.shard_map(
        body,
        mesh=mesh,
        in_specs=(spec, spec, spec, spec, P(), P()),
        out_specs=(spec, P()),
        check_vma=False,
    )
```

```python
import functools
import math

import jax
import jax.numpy as jnp
import numpy as np
from jax import lax
from jax.experimental import pallas as pl
from jax.experimental.pallas import tpu as pltpu
from jax.sharding import PartitionSpec as P

NZ = 32
H = 32
KC = 64
S = 256
REGIONS = 8
ROWS = 8
COLS = 64
PAIRS = NZ // 2
LANES = 128
GROUPS = ROWS * COLS // LANES
CELLS = ROWS * COLS
WIDTH = NZ * KC

base_freq = 0.1
norm_eps = 1e-06

GX = 0
GYP = GX + GROUPS + 1
GYM = GYP + GROUPS
GZP = GYM + GROUPS
GZM = GZP + GROUPS
CAP = GZM + GROUPS
DIO = CAP + GROUPS
GSUM = DIO + GROUPS
FIELDS = GSUM + GROUPS

UNROLL = 2
PACK_MIB = 46

CHUNK = 64


def halves(table):
    high = table.astype(jnp.bfloat16)
    low = (table - high.astype(np.float64)).astype(jnp.bfloat16)
    return high, low


def constant_tables():
    orders = np.arange(1, H + 1, dtype=np.float64)
    angles = orders[:, None] * (2.0 * math.pi * np.arange(S) / S)[None, :]
    cosines, sines = np.cos(angles), np.sin(angles)
    synthesis = np.concatenate([cosines, sines], axis=0)
    high, low = halves(synthesis.T)
    forward = np.concatenate([high, low, high, low], axis=1)
    scaled = base_freq * orders[:, None]
    from_even = halves(synthesis / S)
    from_odd = halves(np.concatenate([scaled * sines, -scaled * cosines], axis=0) / S)
    rows = []
    for part in range(2):
        blocks = []
        for first in range(0, S, CHUNK):
            even = from_even[part][:, first : first + CHUNK]
            odd = from_odd[part][:, first : first + CHUNK]
            blocks += [even, even, odd, odd]
        rows.append(np.concatenate(blocks, axis=1))
    backward = np.concatenate(rows, axis=0).astype(np.float32)
    rates = np.concatenate([scaled, -scaled], axis=0).astype(np.float32)
    rates = np.ascontiguousarray(np.broadcast_to(rates, (KC, LANES)))
    spread = np.zeros((2 * ROWS, CELLS), np.float32)
    for row in range(ROWS):
        group, half = row % GROUPS, row // GROUPS
        spread[row, group * LANES + half * COLS] = 1.0
        spread[ROWS + row, group * LANES + half * COLS + COLS - 1] = 1.0
    widen = np.tile(np.repeat(np.eye(NZ), KC, axis=1), (3, 1)).astype(jnp.bfloat16)
    return forward, backward, rates, spread, widen


def split(values):
    high = values.astype(jnp.bfloat16)
    low = (values - high.astype(jnp.float32)).astype(jnp.bfloat16)
    return high, low


def dot(left, right):
    return jnp.dot(left, right, preferred_element_type=jnp.float32)


def dot_exact(left, right):
    return jnp.dot(
        left, right, preferred_element_type=jnp.float32, precision=lax.Precision.HIGHEST
    )


def harmonic_mean(left, right):
    return 2.0 * left * right / (left + right)


def look_up(region, table_ref):
    found = jnp.zeros(region.shape, jnp.float32)
    for index in range(REGIONS):
        found = jnp.where(region == float(index), table_ref[index], found)
    return found


def in_groups(block, group):
    return jnp.concatenate([block[group], block[group + GROUPS]], axis=0)


def layers_of(ref, pair):
    lanes = pl.ds(pl.multiple_of(pair * LANES, LANES), LANES)
    return ref.at[..., lanes]


def group_lanes(g):
    return slice(g * LANES, (g + 1) * LANES)


def sampled(volt, forward):
    high, low = split(volt)
    return dot(forward, jnp.concatenate([high, high, low, low], axis=0))


def bend(samples, bent):
    for first in range(0, S, CHUNK):
        sample = samples[first : first + CHUNK]
        odd = jnp.tanh(sample)
        even = jnp.abs(sample) - jnp.log(1.0 + jnp.abs(odd))
        coarse = jnp.round(even)
        near = odd.astype(jnp.bfloat16).astype(jnp.float32)
        for index, term in enumerate((coarse, even - coarse, near, odd - near)):
            row = 4 * first + index * CHUNK
            bent[row : row + CHUNK] = term


def diode_kernel(volt_ref, forward_ref, backward_ref, turned, diode_ref, *scratch):
    samples, bents = scratch[:2], scratch[2:]

    def turn(pair):
        block = layers_of(volt_ref, pair)
        for g in range(GROUPS):
            turned[pair, :, group_lanes(g)] = in_groups(block, g).T

    def sample(pair, half):
        mine = slice(half * KC, (half + 1) * KC)
        samples[half][...] = sampled(turned[pair, mine, :], forward_ref[...])

    def project(pair, half):
        mine = slice(half * KC, (half + 1) * KC)
        spectrum = dot(backward_ref[...], bents[half][...])
        diode_ref[pair, mine, :] = spectrum[:KC] + spectrum[KC:]

    turn(0)
    turn(1)
    sample(0, 0)
    bents[1][...] = jnp.zeros(bents[1].shape, jnp.float32)

    def at_pair(pair):
        sample(pair, 1)
        project(jnp.maximum(pair - 1, 0), 1)
        bend(samples[0], bents[0])
        sample(jnp.minimum(pair + 1, PAIRS - 1), 0)
        bend(samples[1], bents[1])
        project(pair, 0)
        turn(jnp.minimum(pair + 2, PAIRS - 1))

    @pl.loop(0, PAIRS // UNROLL)
    def _(block):
        for index in range(UNROLL):
            at_pair(UNROLL * block + index)

    project(PAIRS - 1, 1)


def beside(block, group):
    return jnp.concatenate([block[group], block[group + GROUPS]], axis=1).astype(jnp.float32)


def kinds_of(message):
    return message[:, WIDTH : WIDTH + NZ] - 1.0


def fill_factors(sigma_ref, cap_ref, region_ref, mask_ref, rows, cols, own_cols, spread, factors):
    lane = lax.broadcasted_iota(jnp.int32, (NZ, LANES), 1)
    first = lane < COLS
    column = jnp.where(first, lane, lane - COLS)
    region = [beside(region_ref, g) for g in range(GROUPS)]
    conduct = [look_up(r, sigma_ref) for r in region]
    row_kinds = jnp.concatenate(rows, axis=0).T
    row_halo = look_up(row_kinds[:NZ] - 1.0, sigma_ref)
    outer = look_up(jnp.concatenate([kinds_of(m) for m in cols], axis=0), sigma_ref)
    inner = look_up(jnp.concatenate([kinds_of(m) for m in own_cols], axis=0), sigma_ref)
    rim = harmonic_mean(inner, outer)
    rim_spread = dot_exact(rim.T, spread)
    below = jnp.where(first, row_halo, pltpu.roll(conduct[GROUPS - 1], COLS, 1))
    above = jnp.where(first, pltpu.roll(conduct[0], COLS, 1), row_halo)
    stack = [below] + conduct + [above]
    faces = [harmonic_mean(stack[g], stack[g + 1]) for g in range(GROUPS + 1)]
    layer = lax.broadcasted_iota(jnp.int32, (NZ, LANES), 0)
    for g in range(GROUPS + 1):
        factors[GX + g] = faces[g]
    for g in range(GROUPS):
        here = conduct[g]
        plus = harmonic_mean(here, pltpu.roll(here, LANES - 1, 1))
        plus = jnp.where(column == COLS - 1, 0.0, plus)
        minus = jnp.where(column == 0, 0.0, harmonic_mean(here, pltpu.roll(here, 1, 1)))
        upper = harmonic_mean(here, pltpu.roll(here, NZ - 1, 0))
        upper = jnp.where(layer == NZ - 1, 0.0, upper)
        lower = jnp.where(layer == 0, 0.0, harmonic_mean(here, pltpu.roll(here, 1, 0)))
        diode = beside(mask_ref, g)
        factors[GYP + g] = plus
        factors[GYM + g] = minus
        factors[GZP + g] = upper
        factors[GZM + g] = lower
        factors[CAP + g] = look_up(region[g], cap_ref)
        factors[DIO + g] = diode
        factors[GSUM + g] = (
            faces[g] + faces[g + 1] + plus + minus + rim_spread[:, group_lanes(g)]
            + upper + lower + 0.5 * diode
        )
    return rim


def residual_kernel(
    sigma_ref,
    cap_ref,
    turned,
    diode_ref,
    drive_ref,
    region_ref,
    mask_ref,
    row_near,
    row_far,
    col_near,
    col_far,
    own_near,
    own_far,
    rates_ref,
    spread_ref,
    widen_ref,
    out_ref,
    squares_ref,
    factors,
    rim_flux,
    *scratch,
):
    sums, ready, sent = scratch[:2], scratch[2], scratch[3]
    up, down = is_even("gx"), is_even("gy")

    def low_high(even, near, far):
        return [jnp.where(even, far, near), jnp.where(even, near, far)]

    cols = low_high(down, col_near[...], col_far[...])
    rim = fill_factors(
        sigma_ref,
        cap_ref,
        region_ref,
        mask_ref,
        low_high(up, row_near[:, WIDTH:], row_far[:, WIDTH:]),
        cols,
        low_high(down, own_near[...], own_far[...]),
        spread_ref[...],
        factors,
    )
    top = rim.astype(jnp.bfloat16).astype(jnp.float32)
    middle = (rim - top).astype(jnp.bfloat16).astype(jnp.float32)
    rim = jnp.concatenate([top, middle, rim - top - middle], axis=1).astype(jnp.bfloat16)
    rim_flux[...] = dot(rim, widen_ref[...]) * jnp.concatenate([c[:, :WIDTH] for c in cols], axis=0)
    first = lax.broadcasted_iota(jnp.int32, (KC, LANES), 1) < COLS
    at_low = lax.broadcasted_iota(jnp.int32, (8, LANES), 0) == 0
    at_high = lax.broadcasted_iota(jnp.int32, (8, LANES), 0) == 7

    def gather(pair, slot):
        row_halo = jnp.concatenate(
            low_high(up, layers_of(row_near, pair)[...], layers_of(row_far, pair)[...]), axis=0
        ).T
        for half in range(2):
            layer = 2 * pair + half
            mine = slice(half * KC, (half + 1) * KC)
            other = slice((1 - half) * KC, (2 - half) * KC)
            before = jnp.maximum(pair - 1, 0) if half == 0 else pair
            after = pair if half == 0 else jnp.minimum(pair + 1, PAIRS - 1)

            def factor(index):
                return factors[index, pl.ds(layer, 1), :]

            volts = [turned[pair, mine, group_lanes(g)] for g in range(GROUPS)]
            halo = row_halo[mine]
            below = jnp.where(first, halo, pltpu.roll(volts[GROUPS - 1], COLS, 1))
            above = jnp.where(first, pltpu.roll(volts[0], COLS, 1), halo)
            stack = [below] + volts + [above]
            for g in range(GROUPS):
                here = volts[g]
                swapped = jnp.concatenate([here[KC // 2 :], here[: KC // 2]], axis=0)
                total = factor(GSUM + g) * here
                total -= factor(GX + g) * stack[g]
                total -= factor(GX + g + 1) * stack[g + 2]
                total -= factor(GYP + g) * pltpu.roll(here, LANES - 1, 1)
                total -= factor(GYM + g) * pltpu.roll(here, 1, 1)
                total -= factor(GZP + g) * turned[after, other, group_lanes(g)]
                total -= factor(GZM + g) * turned[before, other, group_lanes(g)]
                total += factor(CAP + g) * rates_ref[...] * swapped
                total += factor(DIO + g) * diode_ref[pair, mine, group_lanes(g)]
                sums[slot][mine, group_lanes(g)] = total

    def copy_out(pair):
        return pltpu.make_async_copy(ready.at[pair], layers_of(out_ref, pair), sent.at[pair])

    def finish(pair, slot, squares):
        drive = layers_of(drive_ref, pair)
        edges = layers_of(rim_flux, pair)
        for g in range(GROUPS):
            cells = sums[slot][:, group_lanes(g)].T
            for which in range(2):
                row = g + which * GROUPS
                value = cells[which * COLS : (which + 1) * COLS] - drive[row]
                low = jnp.where(at_low, edges[row : row + 1, :], 0.0)
                high = jnp.where(at_high, edges[ROWS + row : ROWS + row + 1, :], 0.0)
                value = jnp.concatenate(
                    [value[:8] - low, value[8 : COLS - 8], value[COLS - 8 :] - high], axis=0
                )
                ready[pair, row] = value
                squares += jnp.sum((value * value).reshape(COLS // 8, 8, LANES), axis=0)
        return squares

    for slot in range(2):
        gather(slot, slot)

    def step(index, squares):
        pair = 2 * index
        for slot in range(2):
            squares = finish(pair - 2 + slot, slot, squares)
            gather(pair + slot, slot)
        for slot in range(2):
            copy_out(pair - 2 + slot).start()
        return squares

    squares = lax.fori_loop(1, PAIRS // 2, step, jnp.zeros((8, LANES), jnp.float32))
    for slot in range(2):
        squares = finish(PAIRS - 2 + slot, slot, squares)
        copy_out(PAIRS - 2 + slot).start()
    squares = jnp.sum(squares, axis=0, keepdims=True)
    squares += pltpu.roll(squares, KC, 1)
    squares_ref[...] = jnp.broadcast_to(squares, squares_ref.shape)
    for pair in range(PAIRS):
        copy_out(pair).wait()


def in_vmem(count):
    return [pl.BlockSpec(memory_space=pltpu.VMEM)] * count


def is_even(axis):
    return lax.rem(lax.axis_index(axis), 2) == 0


def pack_kernel(volt_hbm, region_hbm, *refs):
    row_near, row_far, col_near, col_far, volt_ref, region_ref, arrived = refs
    fetches = [
        pltpu.make_async_copy(volt_hbm.at[row], volt_ref.at[row], arrived.at[row])
        for row in range(ROWS)
    ]
    fetches.append(pltpu.make_async_copy(region_hbm, region_ref, arrived.at[ROWS]))
    for fetch in reversed(fetches):
        fetch.start()
    fetches[ROWS].wait()
    def put(message, volts, regions):
        message[:, :WIDTH] = volts
        padding = jnp.zeros((regions.shape[0], LANES - NZ), jnp.float32)
        message[:, WIDTH:] = jnp.concatenate([regions, padding], axis=1)

    for row in reversed(range(ROWS)):
        fetches[row].wait()
    def kinds_at(row):
        return region_ref[row].astype(jnp.float32).T + 1.0

    kinds = [kinds_at(row) for row in range(ROWS)]
    up, down = is_even("gx"), is_even("gy")
    for message, row in (
        (row_near, jnp.where(up, ROWS - 1, 0)),
        (row_far, jnp.where(up, 0, ROWS - 1)),
    ):
        put(message, volt_ref[row], kinds_at(row))
    sides = [
        (volt_ref[:, col, :], jnp.concatenate([kind[col : col + 1] for kind in kinds], axis=0))
        for col in (0, COLS - 1)
    ]
    for message, even, odd in ((col_near, sides[1], sides[0]), (col_far, sides[0], sides[1])):
        put(message, *(jnp.where(down, e, o) for e, o in zip(even, odd)))


def packed(volt, region):
    shapes = [(COLS, WIDTH + LANES)] * 2 + [(ROWS, WIDTH + LANES)] * 2 + [volt.shape]
    return pl.pallas_call(
        pack_kernel,
        in_specs=[pl.BlockSpec(memory_space=pltpu.HBM)] * 2,
        out_specs=in_vmem(5),
        out_shape=[jax.ShapeDtypeStruct(shape, jnp.float32) for shape in shapes],
        scratch_shapes=[
            pltpu.VMEM(region.shape, region.dtype),
            pltpu.SemaphoreType.DMA((ROWS + 1,)),
        ],
        compiler_params=pltpu.CompilerParams(vmem_limit_bytes=PACK_MIB * 1024 * 1024),
        name="pack",
    )(volt, region)


def diode_part(volt):
    forward, backward = constant_tables()[:2]
    samples = CELLS * NZ * S
    whole = jax.ShapeDtypeStruct((PAIRS, LANES, CELLS), jnp.float32)
    return pl.pallas_call(
        diode_kernel,
        in_specs=in_vmem(3),
        out_specs=in_vmem(2),
        out_shape=[whole, whole],
        scratch_shapes=[pltpu.VMEM((S, CELLS), jnp.float32)] * 2
        + [pltpu.VMEM((4 * S, CELLS), jnp.float32)] * 2,
        compiler_params=pltpu.CompilerParams(vmem_limit_bytes=16 * 1024 * 1024),
        cost_estimate=pl.CostEstimate(
            flops=samples * 1000, bytes_accessed=4 * CELLS * WIDTH, transcendentals=2 * samples
        ),
        name="diode",
    )(volt, jnp.asarray(forward), jnp.asarray(backward))


def whole_residual(turned, diode, drive, region, mask, halos, own_cols, tables, copies):
    rates, spread, widen = constant_tables()[2:]
    smem = pl.BlockSpec(memory_space=pltpu.SMEM)
    return pl.pallas_call(
        residual_kernel,
        in_specs=[smem, smem] + in_vmem(14),
        out_specs=[pl.BlockSpec(memory_space=pltpu.HBM)] + in_vmem(1),
        out_shape=[
            jax.ShapeDtypeStruct((ROWS, COLS, WIDTH), jnp.float32),
            jax.ShapeDtypeStruct((copies, LANES), jnp.float32),
        ],
        scratch_shapes=[
            pltpu.VMEM((FIELDS, NZ, LANES), jnp.float32),
            pltpu.VMEM((2 * ROWS, WIDTH), jnp.float32),
            pltpu.VMEM((LANES, CELLS), jnp.float32),
            pltpu.VMEM((LANES, CELLS), jnp.float32),
            pltpu.VMEM((PAIRS, ROWS, COLS, LANES), jnp.float32),
            pltpu.SemaphoreType.DMA((PAIRS,)),
        ],
        compiler_params=pltpu.CompilerParams(vmem_limit_bytes=16 * 1024 * 1024),
        cost_estimate=pl.CostEstimate(
            flops=30 * CELLS * WIDTH, bytes_accessed=2 * 4 * CELLS * WIDTH, transcendentals=0
        ),
        name="residual",
    )(
        *tables,
        turned,
        diode,
        drive,
        region,
        mask,
        *halos,
        *own_cols,
        jnp.asarray(rates),
        jnp.asarray(spread),
        jnp.asarray(widen),
    )


def swapped_halos(near, far, axis, periodic):
    count = lax.axis_size(axis)
    close = [(i, i ^ 1) for i in range(count)]
    apart = [(i, i + 1 if i % 2 else i - 1) for i in range(count)]
    if periodic:
        apart = [(source, target % count) for source, target in apart]
    apart = [(source, target) for source, target in apart if 0 <= target < count]
    return lax.ppermute(near, axis, close), lax.ppermute(far, axis, apart)


def exchanged_sum(copies, axis):
    return jnp.sum(lax.all_to_all(copies, axis, 0, 0, tiled=True), axis=0)


def body(volt, drive, region, diode_mask, sigma_table, cap_table):
    by_layer = jnp.transpose(region, (0, 2, 1))
    mask = jnp.transpose(diode_mask, (0, 2, 1))
    row_near, row_far, col_near, col_far, volt = packed(volt, by_layer)
    rows = swapped_halos(row_near, row_far, "gx", True)
    cols = swapped_halos(col_near, col_far, "gy", False)
    turned, diode = diode_part(volt)
    nx, ny = lax.axis_size("gx"), lax.axis_size("gy")
    residual, squares = whole_residual(
        turned,
        diode,
        drive,
        by_layer,
        mask,
        rows + cols,
        (col_near, col_far),
        (sigma_table, cap_table),
        nx,
    )
    over_x = exchanged_sum(squares, "gx")
    summed = exchanged_sum(jnp.broadcast_to(over_x, (ny, LANES)), "gy")[:KC]
    return residual, jnp.sqrt(summed / (CELLS * NZ * nx * ny) + norm_eps)


def solution(mesh):
    spec = P("gx", "gy", None)
    return jax.shard_map(
        body,
        mesh=mesh,
        in_specs=(spec, spec, spec, spec, P(), P()),
        out_specs=(spec, P()),
        check_vma=False,
    )
```

```python
import functools
import math

import jax
import jax.numpy as jnp
import numpy as np
from jax import lax
from jax.experimental import pallas as pl
from jax.experimental.pallas import tpu as pltpu
from jax.sharding import PartitionSpec as P

NZ = 32
H = 32
KC = 64
S = 256
REGIONS = 8
ROWS = 8
COLS = 64
PAIRS = NZ // 2
LANES = 128
GROUPS = ROWS * COLS // LANES
CELLS = ROWS * COLS
WIDTH = NZ * KC

base_freq = 0.1
norm_eps = 1e-06

GX = 0
GYP = GX + GROUPS + 1
GYM = GYP + GROUPS
GZP = GYM + GROUPS
GZM = GZP + GROUPS
CAP = GZM + GROUPS
DIO = CAP + GROUPS
GSUM = DIO + GROUPS
FIELDS = GSUM + GROUPS

UNROLL = 4
PACK_MIB = 8

CHUNK = 64


def halves(table):
    high = table.astype(jnp.bfloat16)
    low = (table - high.astype(np.float64)).astype(jnp.bfloat16)
    return high, low


def constant_tables():
    orders = np.arange(1, H + 1, dtype=np.float64)
    angles = orders[:, None] * (2.0 * math.pi * np.arange(S) / S)[None, :]
    cosines, sines = np.cos(angles), np.sin(angles)
    synthesis = np.concatenate([cosines, sines], axis=0)
    high, low = halves(synthesis.T)
    forward = np.concatenate([high, low, high, low], axis=1)
    scaled = base_freq * orders[:, None]
    from_even = halves(synthesis / S)
    from_odd = halves(np.concatenate([scaled * sines, -scaled * cosines], axis=0) / S)
    rows = []
    for part in range(2):
        blocks = []
        for first in range(0, S, CHUNK):
            even = from_even[part][:, first : first + CHUNK]
            odd = from_odd[part][:, first : first + CHUNK]
            blocks += [even, even, odd, odd]
        rows.append(np.concatenate(blocks, axis=1))
    backward = np.concatenate(rows, axis=0).astype(np.float32)
    rates = np.concatenate([scaled, -scaled], axis=0).astype(np.float32)
    rates = np.ascontiguousarray(np.broadcast_to(rates, (KC, LANES)))
    spread = np.zeros((2 * ROWS, CELLS), np.float32)
    for row in range(ROWS):
        group, half = row % GROUPS, row // GROUPS
        spread[row, group * LANES + half * COLS] = 1.0
        spread[ROWS + row, group * LANES + half * COLS + COLS - 1] = 1.0
    widen = np.tile(np.repeat(np.eye(NZ), KC, axis=1), (3, 1)).astype(jnp.bfloat16)
    return forward, backward, rates, spread, widen


def split(values):
    high = values.astype(jnp.bfloat16)
    low = (values - high.astype(jnp.float32)).astype(jnp.bfloat16)
    return high, low


def dot(left, right):
    return jnp.dot(left, right, preferred_element_type=jnp.float32)


def dot_exact(left, right):
    return jnp.dot(
        left, right, preferred_element_type=jnp.float32, precision=lax.Precision.HIGHEST
    )


def harmonic_mean(left, right):
    return 2.0 * left * right / (left + right)


def look_up(region, table_ref):
    found = jnp.zeros(region.shape, jnp.float32)
    for index in range(REGIONS):
        found = jnp.where(region == float(index), table_ref[index], found)
    return found


def in_groups(block, group):
    return jnp.concatenate([block[group], block[group + GROUPS]], axis=0)


def layers_of(ref, pair):
    lanes = pl.ds(pl.multiple_of(pair * LANES, LANES), LANES)
    return ref.at[..., lanes]


def group_lanes(g):
    return slice(g * LANES, (g + 1) * LANES)


def sampled(volt, forward):
    high, low = split(volt)
    return dot(forward, jnp.concatenate([high, high, low, low], axis=0))


def bend(samples, bent):
    for first in range(0, S, CHUNK):
        sample = samples[first : first + CHUNK]
        odd = jnp.tanh(sample)
        even = jnp.abs(sample) - jnp.log(1.0 + jnp.abs(odd))
        coarse = jnp.round(even)
        near = odd.astype(jnp.bfloat16).astype(jnp.float32)
        for index, term in enumerate((coarse, even - coarse, near, odd - near)):
            row = 4 * first + index * CHUNK
            bent[row : row + CHUNK] = term


def diode_kernel(volt_ref, forward_ref, backward_ref, turned, diode_ref, *scratch):
    samples, bents = scratch[:2], scratch[2:]

    def turn(pair):
        block = layers_of(volt_ref, pair)
        for g in range(GROUPS):
            turned[pair, :, group_lanes(g)] = in_groups(block, g).T

    def sample(pair, half):
        mine = slice(half * KC, (half + 1) * KC)
        samples[half][...] = sampled(turned[pair, mine, :], forward_ref[...])

    def project(pair, half):
        mine = slice(half * KC, (half + 1) * KC)
        spectrum = dot(backward_ref[...], bents[half][...])
        diode_ref[pair, mine, :] = spectrum[:KC] + spectrum[KC:]

    turn(0)
    turn(1)
    sample(0, 0)
    bents[1][...] = jnp.zeros(bents[1].shape, jnp.float32)

    def at_pair(pair):
        sample(pair, 1)
        project(jnp.maximum(pair - 1, 0), 1)
        bend(samples[0], bents[0])
        sample(jnp.minimum(pair + 1, PAIRS - 1), 0)
        bend(samples[1], bents[1])
        project(pair, 0)
        turn(jnp.minimum(pair + 2, PAIRS - 1))

    @pl.loop(0, PAIRS // UNROLL)
    def _(block):
        for index in range(UNROLL):
            at_pair(UNROLL * block + index)

    project(PAIRS - 1, 1)


def beside(block, group):
    return jnp.concatenate([block[group], block[group + GROUPS]], axis=1).astype(jnp.float32)


def kinds_of(message):
    return message[:, WIDTH : WIDTH + NZ] - 1.0


def fill_factors(sigma_ref, cap_ref, region_ref, mask_ref, rows, cols, own_cols, spread, factors):
    lane = lax.broadcasted_iota(jnp.int32, (NZ, LANES), 1)
    first = lane < COLS
    column = jnp.where(first, lane, lane - COLS)
    region = [beside(region_ref, g) for g in range(GROUPS)]
    conduct = [look_up(r, sigma_ref) for r in region]
    row_kinds = jnp.concatenate(rows, axis=0).T
    row_halo = look_up(row_kinds[:NZ] - 1.0, sigma_ref)
    outer = look_up(jnp.concatenate([kinds_of(m) for m in cols], axis=0), sigma_ref)
    inner = look_up(jnp.concatenate([kinds_of(m) for m in own_cols], axis=0), sigma_ref)
    rim = harmonic_mean(inner, outer)
    rim_spread = dot_exact(rim.T, spread)
    below = jnp.where(first, row_halo, pltpu.roll(conduct[GROUPS - 1], COLS, 1))
    above = jnp.where(first, pltpu.roll(conduct[0], COLS, 1), row_halo)
    stack = [below] + conduct + [above]
    faces = [harmonic_mean(stack[g], stack[g + 1]) for g in range(GROUPS + 1)]
    layer = lax.broadcasted_iota(jnp.int32, (NZ, LANES), 0)
    for g in range(GROUPS + 1):
        factors[GX + g] = faces[g]
    for g in range(GROUPS):
        here = conduct[g]
        plus = harmonic_mean(here, pltpu.roll(here, LANES - 1, 1))
        plus = jnp.where(column == COLS - 1, 0.0, plus)
        minus = jnp.where(column == 0, 0.0, harmonic_mean(here, pltpu.roll(here, 1, 1)))
        upper = harmonic_mean(here, pltpu.roll(here, NZ - 1, 0))
        upper = jnp.where(layer == NZ - 1, 0.0, upper)
        lower = jnp.where(layer == 0, 0.0, harmonic_mean(here, pltpu.roll(here, 1, 0)))
        diode = beside(mask_ref, g)
        factors[GYP + g] = plus
        factors[GYM + g] = minus
        factors[GZP + g] = upper
        factors[GZM + g] = lower
        factors[CAP + g] = look_up(region[g], cap_ref)
        factors[DIO + g] = diode
        factors[GSUM + g] = (
            faces[g] + faces[g + 1] + plus + minus + rim_spread[:, group_lanes(g)]
            + upper + lower + 0.5 * diode
        )
    return rim


def residual_kernel(
    sigma_ref,
    cap_ref,
    turned,
    diode_ref,
    drive_ref,
    region_ref,
    mask_ref,
    row_near,
    row_far,
    col_near,
    col_far,
    own_near,
    own_far,
    rates_ref,
    spread_ref,
    widen_ref,
    out_ref,
    squares_ref,
    factors,
    rim_flux,
    *scratch,
):
    sums, ready, sent = scratch[:2], scratch[2], scratch[3]
    up, down = is_even("gx"), is_even("gy")

    def low_high(even, near, far):
        return [jnp.where(even, far, near), jnp.where(even, near, far)]

    cols = low_high(down, col_near[...], col_far[...])
    rim = fill_factors(
        sigma_ref,
        cap_ref,
        region_ref,
        mask_ref,
        low_high(up, row_near[:, WIDTH:], row_far[:, WIDTH:]),
        cols,
        low_high(down, own_near[...], own_far[...]),
        spread_ref[...],
        factors,
    )
    top = rim.astype(jnp.bfloat16).astype(jnp.float32)
    middle = (rim - top).astype(jnp.bfloat16).astype(jnp.float32)
    rim = jnp.concatenate([top, middle, rim - top - middle], axis=1).astype(jnp.bfloat16)
    rim_flux[...] = dot(rim, widen_ref[...]) * jnp.concatenate([c[:, :WIDTH] for c in cols], axis=0)
    first = lax.broadcasted_iota(jnp.int32, (KC, LANES), 1) < COLS
    at_low = lax.broadcasted_iota(jnp.int32, (8, LANES), 0) == 0
    at_high = lax.broadcasted_iota(jnp.int32, (8, LANES), 0) == 7

    def gather(pair, slot):
        row_halo = jnp.concatenate(
            low_high(up, layers_of(row_near, pair)[...], layers_of(row_far, pair)[...]), axis=0
        ).T
        for half in range(2):
            layer = 2 * pair + half
            mine = slice(half * KC, (half + 1) * KC)
            other = slice((1 - half) * KC, (2 - half) * KC)
            before = jnp.maximum(pair - 1, 0) if half == 0 else pair
            after = pair if half == 0 else jnp.minimum(pair + 1, PAIRS - 1)

            def factor(index):
                return factors[index, pl.ds(layer, 1), :]

            volts = [turned[pair, mine, group_lanes(g)] for g in range(GROUPS)]
            halo = row_halo[mine]
            below = jnp.where(first, halo, pltpu.roll(volts[GROUPS - 1], COLS, 1))
            above = jnp.where(first, pltpu.roll(volts[0], COLS, 1), halo)
            stack = [below] + volts + [above]
            for g in range(GROUPS):
                here = volts[g]
                swapped = jnp.concatenate([here[KC // 2 :], here[: KC // 2]], axis=0)
                total = factor(GSUM + g) * here
                total -= factor(GX + g) * stack[g]
                total -= factor(GX + g + 1) * stack[g + 2]
                total -= factor(GYP + g) * pltpu.roll(here, LANES - 1, 1)
                total -= factor(GYM + g) * pltpu.roll(here, 1, 1)
                total -= factor(GZP + g) * turned[after, other, group_lanes(g)]
                total -= factor(GZM + g) * turned[before, other, group_lanes(g)]
                total += factor(CAP + g) * rates_ref[...] * swapped
                total += factor(DIO + g) * diode_ref[pair, mine, group_lanes(g)]
                sums[slot][mine, group_lanes(g)] = total

    def copy_out(pair):
        return pltpu.make_async_copy(ready.at[pair], layers_of(out_ref, pair), sent.at[pair])

    def finish(pair, slot, squares):
        drive = layers_of(drive_ref, pair)
        edges = layers_of(rim_flux, pair)
        for g in range(GROUPS):
            cells = sums[slot][:, group_lanes(g)].T
            for which in range(2):
                row = g + which * GROUPS
                value = cells[which * COLS : (which + 1) * COLS] - drive[row]
                low = jnp.where(at_low, edges[row : row + 1, :], 0.0)
                high = jnp.where(at_high, edges[ROWS + row : ROWS + row + 1, :], 0.0)
                value = jnp.concatenate(
                    [value[:8] - low, value[8 : COLS - 8], value[COLS - 8 :] - high], axis=0
                )
                ready[pair, row] = value
                squares += jnp.sum((value * value).reshape(COLS // 8, 8, LANES), axis=0)
        return squares

    for slot in range(2):
        gather(slot, slot)

    def step(index, squares):
        pair = 2 * index
        for slot in range(2):
            squares = finish(pair - 2 + slot, slot, squares)
            gather(pair + slot, slot)
        for slot in range(2):
            copy_out(pair - 2 + slot).start()
        return squares

    squares = lax.fori_loop(1, PAIRS // 2, step, jnp.zeros((8, LANES), jnp.float32))
    for slot in range(2):
        squares = finish(PAIRS - 2 + slot, slot, squares)
        copy_out(PAIRS - 2 + slot).start()
    squares = jnp.sum(squares, axis=0, keepdims=True)
    squares += pltpu.roll(squares, KC, 1)
    squares_ref[...] = jnp.broadcast_to(squares, squares_ref.shape)
    for pair in range(PAIRS):
        copy_out(pair).wait()


def in_vmem(count):
    return [pl.BlockSpec(memory_space=pltpu.VMEM)] * count


def is_even(axis):
    return lax.rem(lax.axis_index(axis), 2) == 0


def pack_kernel(volt_hbm, region_hbm, table_hbm, *refs):
    row_near, row_far, col_near, col_far, table_ref, sides_ref, region_ref, arrived = refs
    up, down = is_even("gx"), is_even("gy")
    near_row = jnp.where(up, ROWS - 1, 0)
    far_row = ROWS - 1 - near_row
    fetches = [
        pltpu.make_async_copy(region_hbm, region_ref, arrived.at[0]),
        pltpu.make_async_copy(volt_hbm.at[:, 0], sides_ref.at[0], arrived.at[1]),
        pltpu.make_async_copy(volt_hbm.at[:, COLS - 1], sides_ref.at[1], arrived.at[2]),
        pltpu.make_async_copy(
            volt_hbm.at[near_row], row_near.at[:, pl.ds(0, WIDTH)], arrived.at[3]
        ),
        pltpu.make_async_copy(volt_hbm.at[far_row], row_far.at[:, pl.ds(0, WIDTH)], arrived.at[4]),
        pltpu.make_async_copy(table_hbm, table_ref, arrived.at[5]),
    ]
    for fetch in fetches:
        fetch.start()
    fetches[0].wait()

    def kinds_at(row):
        return region_ref[row].astype(jnp.float32).T + 1.0

    def put_kinds(message, regions):
        padding = jnp.zeros((regions.shape[0], LANES - NZ), jnp.float32)
        message[:, WIDTH:] = jnp.concatenate([regions, padding], axis=1)

    kinds = [kinds_at(row) for row in range(ROWS)]
    put_kinds(row_near, kinds_at(near_row))
    put_kinds(row_far, kinds_at(far_row))
    low, high = [
        jnp.concatenate([kind[col : col + 1] for kind in kinds], axis=0) for col in (0, COLS - 1)
    ]
    put_kinds(col_near, jnp.where(down, high, low))
    put_kinds(col_far, jnp.where(down, low, high))
    for fetch in fetches[1:]:
        fetch.wait()
    low, high = sides_ref[0], sides_ref[1]
    col_near[:, :WIDTH] = jnp.where(down, high, low)
    col_far[:, :WIDTH] = jnp.where(down, low, high)


def packed(volt, region, table):
    shapes = [(COLS, WIDTH + LANES)] * 2 + [(ROWS, WIDTH + LANES)] * 2 + [table.shape]
    return pl.pallas_call(
        pack_kernel,
        in_specs=[pl.BlockSpec(memory_space=pltpu.HBM)] * 3,
        out_specs=in_vmem(5),
        out_shape=[jax.ShapeDtypeStruct(shape, jnp.float32) for shape in shapes],
        scratch_shapes=[
            pltpu.VMEM((2, ROWS, WIDTH), jnp.float32),
            pltpu.VMEM(region.shape, region.dtype),
            pltpu.SemaphoreType.DMA((6,)),
        ],
        compiler_params=pltpu.CompilerParams(vmem_limit_bytes=PACK_MIB * 1024 * 1024),
        name="pack",
    )(*(pltpu.with_memory_space_constraint(array, pltpu.HBM) for array in (volt, region, table)))


def diode_part(volt, backward):
    forward = constant_tables()[0]
    samples = CELLS * NZ * S
    whole = jax.ShapeDtypeStruct((PAIRS, LANES, CELLS), jnp.float32)
    return pl.pallas_call(
        diode_kernel,
        in_specs=in_vmem(3),
        out_specs=in_vmem(2),
        out_shape=[whole, whole],
        scratch_shapes=[pltpu.VMEM((S, CELLS), jnp.float32)] * 2
        + [pltpu.VMEM((4 * S, CELLS), jnp.float32)] * 2,
        compiler_params=pltpu.CompilerParams(vmem_limit_bytes=16 * 1024 * 1024),
        cost_estimate=pl.CostEstimate(
            flops=samples * 1000, bytes_accessed=4 * CELLS * WIDTH, transcendentals=2 * samples
        ),
        name="diode",
    )(volt, jnp.asarray(forward), backward)


def whole_residual(turned, diode, drive, region, mask, halos, own_cols, tables, copies):
    rates, spread, widen = constant_tables()[2:]
    smem = pl.BlockSpec(memory_space=pltpu.SMEM)
    return pl.pallas_call(
        residual_kernel,
        in_specs=[smem, smem] + in_vmem(14),
        out_specs=[pl.BlockSpec(memory_space=pltpu.HBM)] + in_vmem(1),
        out_shape=[
            jax.ShapeDtypeStruct((ROWS, COLS, WIDTH), jnp.float32),
            jax.ShapeDtypeStruct((copies, LANES), jnp.float32),
        ],
        scratch_shapes=[
            pltpu.VMEM((FIELDS, NZ, LANES), jnp.float32),
            pltpu.VMEM((2 * ROWS, WIDTH), jnp.float32),
            pltpu.VMEM((LANES, CELLS), jnp.float32),
            pltpu.VMEM((LANES, CELLS), jnp.float32),
            pltpu.VMEM((PAIRS, ROWS, COLS, LANES), jnp.float32),
            pltpu.SemaphoreType.DMA((PAIRS,)),
        ],
        compiler_params=pltpu.CompilerParams(vmem_limit_bytes=16 * 1024 * 1024),
        cost_estimate=pl.CostEstimate(
            flops=30 * CELLS * WIDTH, bytes_accessed=2 * 4 * CELLS * WIDTH, transcendentals=0
        ),
        name="residual",
    )(
        *tables,
        turned,
        diode,
        drive,
        region,
        mask,
        *halos,
        *own_cols,
        jnp.asarray(rates),
        jnp.asarray(spread),
        jnp.asarray(widen),
    )


def swapped_halos(near, far, axis, periodic):
    count = lax.axis_size(axis)
    close = [(i, i ^ 1) for i in range(count)]
    apart = [(i, i + 1 if i % 2 else i - 1) for i in range(count)]
    if periodic:
        apart = [(source, target % count) for source, target in apart]
    apart = [(source, target) for source, target in apart if 0 <= target < count]
    return lax.ppermute(near, axis, close), lax.ppermute(far, axis, apart)


def exchanged_sum(copies, axis):
    return jnp.sum(lax.all_to_all(copies, axis, 0, 0, tiled=True), axis=0)


def body(volt, drive, region, diode_mask, sigma_table, cap_table):
    by_layer = jnp.transpose(region, (0, 2, 1))
    mask = jnp.transpose(diode_mask, (0, 2, 1))
    backward = jnp.asarray(constant_tables()[1])
    row_near, row_far, col_near, col_far, backward = packed(volt, by_layer, backward)
    rows = swapped_halos(row_near, row_far, "gx", True)
    cols = swapped_halos(col_near, col_far, "gy", False)
    turned, diode = diode_part(volt, backward)
    nx, ny = lax.axis_size("gx"), lax.axis_size("gy")
    residual, squares = whole_residual(
        turned,
        diode,
        drive,
        by_layer,
        mask,
        rows + cols,
        (col_near, col_far),
        (sigma_table, cap_table),
        nx,
    )
    over_x = exchanged_sum(squares, "gx")
    summed = exchanged_sum(jnp.broadcast_to(over_x, (ny, LANES)), "gy")[:KC]
    return residual, jnp.sqrt(summed / (CELLS * NZ * nx * ny) + norm_eps)


def solution(mesh):
    spec = P("gx", "gy", None)
    return jax.shard_map(
        body,
        mesh=mesh,
        in_specs=(spec, spec, spec, spec, P(), P()),
        out_specs=(spec, P()),
        check_vma=False,
    )
```

```python
import functools
import math

import jax
import jax.numpy as jnp
import numpy as np
from jax import lax
from jax.experimental import pallas as pl
from jax.experimental.pallas import tpu as pltpu
from jax.sharding import PartitionSpec as P

NZ = 32
H = 32
KC = 64
S = 256
REGIONS = 8
ROWS = 8
COLS = 64
PAIRS = NZ // 2
LANES = 128
GROUPS = ROWS * COLS // LANES
CELLS = ROWS * COLS
WIDTH = NZ * KC

base_freq = 0.1
norm_eps = 1e-06

GX = 0
GYP = GX + GROUPS + 1
GYM = GYP + GROUPS
GZP = GYM + GROUPS
GZM = GZP + GROUPS
CAP = GZM + GROUPS
DIO = CAP + GROUPS
GSUM = DIO + GROUPS
FIELDS = GSUM + GROUPS

UNROLL = 4
PACK_MIB = 8

CHUNK = 64


def halves(table):
    high = table.astype(jnp.bfloat16)
    low = (table - high.astype(np.float64)).astype(jnp.bfloat16)
    return high, low


def constant_tables():
    orders = np.arange(1, H + 1, dtype=np.float64)
    angles = orders[:, None] * (2.0 * math.pi * np.arange(S) / S)[None, :]
    cosines, sines = np.cos(angles), np.sin(angles)
    synthesis = np.concatenate([cosines, sines], axis=0)
    high, low = halves(synthesis.T)
    forward = np.concatenate([high, low, high, low], axis=1)
    scaled = base_freq * orders[:, None]
    from_even = halves(synthesis / S)
    from_odd = halves(np.concatenate([scaled * sines, -scaled * cosines], axis=0) / S)
    rows = []
    for part in range(2):
        blocks = []
        for first in range(0, S, CHUNK):
            even = from_even[part][:, first : first + CHUNK]
            odd = from_odd[part][:, first : first + CHUNK]
            blocks += [even, even, odd, odd]
        rows.append(np.concatenate(blocks, axis=1))
    backward = np.concatenate(rows, axis=0).astype(np.float32)
    rates = np.concatenate([scaled, -scaled], axis=0).astype(np.float32)
    rates = np.ascontiguousarray(np.broadcast_to(rates, (KC, LANES)))
    spread = np.zeros((2 * ROWS, CELLS), np.float32)
    for row in range(ROWS):
        group, half = row % GROUPS, row // GROUPS
        spread[row, group * LANES + half * COLS] = 1.0
        spread[ROWS + row, group * LANES + half * COLS + COLS - 1] = 1.0
    widen = np.tile(np.repeat(np.eye(NZ), KC, axis=1), (3, 1)).astype(jnp.bfloat16)
    return forward, backward, rates, spread, widen


def split(values):
    high = values.astype(jnp.bfloat16)
    low = (values - high.astype(jnp.float32)).astype(jnp.bfloat16)
    return high, low


def dot(left, right):
    return jnp.dot(left, right, preferred_element_type=jnp.float32)


def dot_exact(left, right):
    return jnp.dot(
        left, right, preferred_element_type=jnp.float32, precision=lax.Precision.HIGHEST
    )


def harmonic_mean(left, right):
    return 2.0 * left * right / (left + right)


def look_up(region, table_ref):
    found = jnp.zeros(region.shape, jnp.float32)
    for index in range(REGIONS):
        found = jnp.where(region == float(index), table_ref[index], found)
    return found


def in_groups(block, group):
    return jnp.concatenate([block[group], block[group + GROUPS]], axis=0)


def layers_of(ref, pair):
    lanes = pl.ds(pl.multiple_of(pair * LANES, LANES), LANES)
    return ref.at[..., lanes]


def group_lanes(g):
    return slice(g * LANES, (g + 1) * LANES)


def sampled(volt, forward):
    high, low = split(volt)
    return dot(forward, jnp.concatenate([high, high, low, low], axis=0))


def bend(samples, bent):
    for first in range(0, S, CHUNK):
        sample = samples[first : first + CHUNK]
        odd = jnp.tanh(sample)
        even = jnp.abs(sample) - jnp.log(1.0 + jnp.abs(odd))
        coarse = jnp.round(even)
        near = odd.astype(jnp.bfloat16).astype(jnp.float32)
        for index, term in enumerate((coarse, even - coarse, near, odd - near)):
            row = 4 * first + index * CHUNK
            bent[row : row + CHUNK] = term


def diode_kernel(volt_ref, forward_ref, backward_ref, turned, diode_ref, *scratch):
    samples, bents = scratch[:2], scratch[2:]

    def turn(pair):
        block = layers_of(volt_ref, pair)
        for g in range(GROUPS):
            turned[pair, :, group_lanes(g)] = in_groups(block, g).T

    def sample(pair, half):
        mine = slice(half * KC, (half + 1) * KC)
        samples[half][...] = sampled(turned[pair, mine, :], forward_ref[...])

    def project(pair, half):
        mine = slice(half * KC, (half + 1) * KC)
        spectrum = dot(backward_ref[...], bents[half][...])
        diode_ref[pair, mine, :] = spectrum[:KC] + spectrum[KC:]

    turn(0)
    turn(1)
    sample(0, 0)
    bents[1][...] = jnp.zeros(bents[1].shape, jnp.float32)

    def at_pair(pair):
        sample(pair, 1)
        project(jnp.maximum(pair - 1, 0), 1)
        bend(samples[0], bents[0])
        sample(jnp.minimum(pair + 1, PAIRS - 1), 0)
        bend(samples[1], bents[1])
        project(pair, 0)
        turn(jnp.minimum(pair + 2, PAIRS - 1))

    @pl.loop(0, PAIRS // UNROLL)
    def _(block):
        for index in range(UNROLL):
            at_pair(UNROLL * block + index)

    project(PAIRS - 1, 1)


def beside(block, group):
    return jnp.concatenate([block[group], block[group + GROUPS]], axis=1).astype(jnp.float32)


def kinds_of(message):
    return message[:, WIDTH : WIDTH + NZ] - 1.0


def fill_factors(sigma_ref, cap_ref, region_ref, mask_ref, rows, cols, own_cols, spread, factors):
    lane = lax.broadcasted_iota(jnp.int32, (NZ, LANES), 1)
    first = lane < COLS
    column = jnp.where(first, lane, lane - COLS)
    region = [beside(region_ref, g) for g in range(GROUPS)]
    conduct = [look_up(r, sigma_ref) for r in region]
    row_kinds = jnp.concatenate(rows, axis=0).T
    row_halo = look_up(row_kinds[:NZ] - 1.0, sigma_ref)
    outer = look_up(jnp.concatenate([kinds_of(m) for m in cols], axis=0), sigma_ref)
    inner = look_up(jnp.concatenate([kinds_of(m) for m in own_cols], axis=0), sigma_ref)
    rim = harmonic_mean(inner, outer)
    rim_spread = dot_exact(rim.T, spread)
    below = jnp.where(first, row_halo, pltpu.roll(conduct[GROUPS - 1], COLS, 1))
    above = jnp.where(first, pltpu.roll(conduct[0], COLS, 1), row_halo)
    stack = [below] + conduct + [above]
    faces = [harmonic_mean(stack[g], stack[g + 1]) for g in range(GROUPS + 1)]
    layer = lax.broadcasted_iota(jnp.int32, (NZ, LANES), 0)
    for g in range(GROUPS + 1):
        factors[GX + g] = faces[g]
    for g in range(GROUPS):
        here = conduct[g]
        plus = harmonic_mean(here, pltpu.roll(here, LANES - 1, 1))
        plus = jnp.where(column == COLS - 1, 0.0, plus)
        minus = jnp.where(column == 0, 0.0, harmonic_mean(here, pltpu.roll(here, 1, 1)))
        upper = harmonic_mean(here, pltpu.roll(here, NZ - 1, 0))
        upper = jnp.where(layer == NZ - 1, 0.0, upper)
        lower = jnp.where(layer == 0, 0.0, harmonic_mean(here, pltpu.roll(here, 1, 0)))
        diode = beside(mask_ref, g)
        factors[GYP + g] = plus
        factors[GYM + g] = minus
        factors[GZP + g] = upper
        factors[GZM + g] = lower
        factors[CAP + g] = look_up(region[g], cap_ref)
        factors[DIO + g] = diode
        factors[GSUM + g] = (
            faces[g] + faces[g + 1] + plus + minus + rim_spread[:, group_lanes(g)]
            + upper + lower + 0.5 * diode
        )
    return rim


def residual_kernel(
    sigma_ref,
    cap_ref,
    turned,
    diode_ref,
    drive_ref,
    region_ref,
    mask_ref,
    row_near,
    row_far,
    col_near,
    col_far,
    own_near,
    own_far,
    rates_ref,
    spread_ref,
    widen_ref,
    out_ref,
    squares_ref,
    factors,
    rim_flux,
    *scratch,
):
    sums, ready, sent = scratch[:2], scratch[2], scratch[3]
    up, down = is_even("gx"), is_even("gy")

    def low_high(even, near, far):
        return [jnp.where(even, far, near), jnp.where(even, near, far)]

    cols = low_high(down, col_near[...], col_far[...])
    rim = fill_factors(
        sigma_ref,
        cap_ref,
        region_ref,
        mask_ref,
        low_high(up, row_near[:, WIDTH:], row_far[:, WIDTH:]),
        cols,
        low_high(down, own_near[...], own_far[...]),
        spread_ref[...],
        factors,
    )
    top = rim.astype(jnp.bfloat16).astype(jnp.float32)
    middle = (rim - top).astype(jnp.bfloat16).astype(jnp.float32)
    rim = jnp.concatenate([top, middle, rim - top - middle], axis=1).astype(jnp.bfloat16)
    rim_flux[...] = dot(rim, widen_ref[...]) * jnp.concatenate([c[:, :WIDTH] for c in cols], axis=0)
    first = lax.broadcasted_iota(jnp.int32, (KC, LANES), 1) < COLS
    at_low = lax.broadcasted_iota(jnp.int32, (8, LANES), 0) == 0
    at_high = lax.broadcasted_iota(jnp.int32, (8, LANES), 0) == 7

    def gather(pair, slot):
        row_halo = jnp.concatenate(
            low_high(up, layers_of(row_near, pair)[...], layers_of(row_far, pair)[...]), axis=0
        ).T
        for half in range(2):
            layer = 2 * pair + half
            mine = slice(half * KC, (half + 1) * KC)
            other = slice((1 - half) * KC, (2 - half) * KC)
            before = jnp.maximum(pair - 1, 0) if half == 0 else pair
            after = pair if half == 0 else jnp.minimum(pair + 1, PAIRS - 1)

            def factor(index):
                return factors[index, pl.ds(layer, 1), :]

            volts = [turned[pair, mine, group_lanes(g)] for g in range(GROUPS)]
            halo = row_halo[mine]
            below = jnp.where(first, halo, pltpu.roll(volts[GROUPS - 1], COLS, 1))
            above = jnp.where(first, pltpu.roll(volts[0], COLS, 1), halo)
            stack = [below] + volts + [above]
            for g in range(GROUPS):
                here = volts[g]
                swapped = jnp.concatenate([here[KC // 2 :], here[: KC // 2]], axis=0)
                total = factor(GSUM + g) * here
                total -= factor(GX + g) * stack[g]
                total -= factor(GX + g + 1) * stack[g + 2]
                total -= factor(GYP + g) * pltpu.roll(here, LANES - 1, 1)
                total -= factor(GYM + g) * pltpu.roll(here, 1, 1)
                total -= factor(GZP + g) * turned[after, other, group_lanes(g)]
                total -= factor(GZM + g) * turned[before, other, group_lanes(g)]
                total += factor(CAP + g) * rates_ref[...] * swapped
                total += factor(DIO + g) * diode_ref[pair, mine, group_lanes(g)]
                sums[slot][mine, group_lanes(g)] = total

    def copy_out(pair):
        return pltpu.make_async_copy(ready.at[pair], layers_of(out_ref, pair), sent.at[pair])

    def finish(pair, slot, squares):
        drive = layers_of(drive_ref, pair)
        edges = layers_of(rim_flux, pair)
        for g in range(GROUPS):
            cells = sums[slot][:, group_lanes(g)].T
            for which in range(2):
                row = g + which * GROUPS
                value = cells[which * COLS : (which + 1) * COLS] - drive[row]
                low = jnp.where(at_low, edges[row : row + 1, :], 0.0)
                high = jnp.where(at_high, edges[ROWS + row : ROWS + row + 1, :], 0.0)
                value = jnp.concatenate(
                    [value[:8] - low, value[8 : COLS - 8], value[COLS - 8 :] - high], axis=0
                )
                ready[pair, row] = value
                squares += jnp.sum((value * value).reshape(COLS // 8, 8, LANES), axis=0)
        return squares

    for slot in range(2):
        gather(slot, slot)

    def step(index, squares):
        pair = 2 * index
        for slot in range(2):
            squares = finish(pair - 2 + slot, slot, squares)
            gather(pair + slot, slot)
        for slot in range(2):
            copy_out(pair - 2 + slot).start()
        return squares

    squares = lax.fori_loop(1, PAIRS // 2, step, jnp.zeros((8, LANES), jnp.float32))
    for slot in range(2):
        squares = finish(PAIRS - 2 + slot, slot, squares)
        copy_out(PAIRS - 2 + slot).start()
    squares = jnp.sum(squares, axis=0, keepdims=True)
    squares += pltpu.roll(squares, KC, 1)
    squares_ref[...] = jnp.broadcast_to(squares, squares_ref.shape)
    for pair in range(PAIRS):
        copy_out(pair).wait()


def in_vmem(count):
    return [pl.BlockSpec(memory_space=pltpu.VMEM)] * count


def is_even(axis):
    return lax.rem(lax.axis_index(axis), 2) == 0


def pack_kernel(volt_hbm, region_hbm, table_hbm, *refs):
    row_near, row_far, col_near, col_far, table_ref, sides_ref, region_ref, arrived = refs
    up, down = is_even("gx"), is_even("gy")
    near_row = jnp.where(up, ROWS - 1, 0)
    far_row = ROWS - 1 - near_row
    fetches = [
        pltpu.make_async_copy(region_hbm, region_ref, arrived.at[0]),
        pltpu.make_async_copy(volt_hbm.at[:, 0], sides_ref.at[0], arrived.at[1]),
        pltpu.make_async_copy(volt_hbm.at[:, COLS - 1], sides_ref.at[1], arrived.at[2]),
        pltpu.make_async_copy(
            volt_hbm.at[near_row], row_near.at[:, pl.ds(0, WIDTH)], arrived.at[3]
        ),
        pltpu.make_async_copy(volt_hbm.at[far_row], row_far.at[:, pl.ds(0, WIDTH)], arrived.at[4]),
        pltpu.make_async_copy(table_hbm, table_ref, arrived.at[5]),
    ]
    for fetch in fetches:
        fetch.start()
    fetches[0].wait()

    def kinds_at(row):
        return region_ref[row].astype(jnp.float32).T + 1.0

    def put_kinds(message, regions):
        padding = jnp.zeros((regions.shape[0], LANES - NZ), jnp.float32)
        message[:, WIDTH:] = jnp.concatenate([regions, padding], axis=1)

    kinds = [kinds_at(row) for row in range(ROWS)]
    put_kinds(row_near, kinds_at(near_row))
    put_kinds(row_far, kinds_at(far_row))
    low, high = [
        jnp.concatenate([kind[col : col + 1] for kind in kinds], axis=0) for col in (0, COLS - 1)
    ]
    put_kinds(col_near, jnp.where(down, high, low))
    put_kinds(col_far, jnp.where(down, low, high))
    for fetch in fetches[1:]:
        fetch.wait()
    low, high = sides_ref[0], sides_ref[1]
    col_near[:, :WIDTH] = jnp.where(down, high, low)
    col_far[:, :WIDTH] = jnp.where(down, low, high)


def packed(volt, region, table):
    shapes = [(COLS, WIDTH + LANES)] * 2 + [(ROWS, WIDTH + LANES)] * 2 + [table.shape]
    return pl.pallas_call(
        pack_kernel,
        in_specs=[pl.BlockSpec(memory_space=pltpu.HBM)] * 3,
        out_specs=in_vmem(5),
        out_shape=[jax.ShapeDtypeStruct(shape, jnp.float32) for shape in shapes],
        scratch_shapes=[
            pltpu.VMEM((2, ROWS, WIDTH), jnp.float32),
            pltpu.VMEM(region.shape, region.dtype),
            pltpu.SemaphoreType.DMA((6,)),
        ],
        compiler_params=pltpu.CompilerParams(vmem_limit_bytes=PACK_MIB * 1024 * 1024),
        name="pack",
    )(*(pltpu.with_memory_space_constraint(array, pltpu.HBM) for array in (volt, region, table)))


def diode_part(volt, backward):
    forward = constant_tables()[0]
    samples = CELLS * NZ * S
    whole = jax.ShapeDtypeStruct((PAIRS, LANES, CELLS), jnp.float32)
    return pl.pallas_call(
        diode_kernel,
        in_specs=in_vmem(3),
        out_specs=in_vmem(2),
        out_shape=[whole, whole],
        scratch_shapes=[pltpu.VMEM((S, CELLS), jnp.float32)] * 2
        + [pltpu.VMEM((4 * S, CELLS), jnp.float32)] * 2,
        compiler_params=pltpu.CompilerParams(vmem_limit_bytes=16 * 1024 * 1024),
        cost_estimate=pl.CostEstimate(
            flops=samples * 1000, bytes_accessed=4 * CELLS * WIDTH, transcendentals=2 * samples
        ),
        name="diode",
    )(volt, jnp.asarray(forward), backward)


def whole_residual(turned, diode, drive, region, mask, halos, own_cols, tables, copies):
    rates, spread, widen = constant_tables()[2:]
    smem = pl.BlockSpec(memory_space=pltpu.SMEM)
    return pl.pallas_call(
        residual_kernel,
        in_specs=[smem, smem] + in_vmem(14),
        out_specs=[pl.BlockSpec(memory_space=pltpu.HBM)] + in_vmem(1),
        out_shape=[
            jax.ShapeDtypeStruct((ROWS, COLS, WIDTH), jnp.float32),
            jax.ShapeDtypeStruct((copies, LANES), jnp.float32),
        ],
        scratch_shapes=[
            pltpu.VMEM((FIELDS, NZ, LANES), jnp.float32),
            pltpu.VMEM((2 * ROWS, WIDTH), jnp.float32),
            pltpu.VMEM((LANES, CELLS), jnp.float32),
            pltpu.VMEM((LANES, CELLS), jnp.float32),
            pltpu.VMEM((PAIRS, ROWS, COLS, LANES), jnp.float32),
            pltpu.SemaphoreType.DMA((PAIRS,)),
        ],
        compiler_params=pltpu.CompilerParams(vmem_limit_bytes=16 * 1024 * 1024),
        cost_estimate=pl.CostEstimate(
            flops=30 * CELLS * WIDTH, bytes_accessed=2 * 4 * CELLS * WIDTH, transcendentals=0
        ),
        name="residual",
    )(
        *tables,
        turned,
        diode,
        drive,
        region,
        mask,
        *halos,
        *own_cols,
        jnp.asarray(rates),
        jnp.asarray(spread),
        jnp.asarray(widen),
    )


def swapped_halos(near, far, axis, periodic):
    count = lax.axis_size(axis)
    close = [(i, i ^ 1) for i in range(count)]
    apart = [(i, i + 1 if i % 2 else i - 1) for i in range(count)]
    if periodic:
        apart = [(source, target % count) for source, target in apart]
    apart = [(source, target) for source, target in apart if 0 <= target < count]
    return lax.ppermute(near, axis, close), lax.ppermute(far, axis, apart)


def exchanged_sum(copies, axis):
    return jnp.sum(lax.all_to_all(copies, axis, 0, 0, tiled=True), axis=0)


def body(volt, drive, region, diode_mask, sigma_table, cap_table):
    by_layer = jnp.transpose(region, (0, 2, 1))
    mask = jnp.transpose(diode_mask, (0, 2, 1))
    backward = jnp.asarray(constant_tables()[1])
    row_near, row_far, col_near, col_far, backward = packed(volt, by_layer, backward)
    rows = swapped_halos(row_near, row_far, "gx", True)
    cols = swapped_halos(col_near, col_far, "gy", False)
    turned, diode = diode_part(volt, backward)
    nx, ny = lax.axis_size("gx"), lax.axis_size("gy")
    residual, squares = whole_residual(
        turned,
        diode,
        drive,
        by_layer,
        mask,
        rows + cols,
        (col_near, col_far),
        (sigma_table, cap_table),
        nx * ny,
    )
    summed = exchanged_sum(squares, ("gx", "gy"))[:KC]
    return residual, jnp.sqrt(summed / (CELLS * NZ * nx * ny) + norm_eps)


def solution(mesh):
    spec = P("gx", "gy", None)
    return jax.shard_map(
        body,
        mesh=mesh,
        in_specs=(spec, spec, spec, spec, P(), P()),
        out_specs=(spec, P()),
        check_vma=False,
    )
```
